128 devices in a mesh: region: 4 (over z_hi, core), tile: 32 (over x, y, z_lo).
Axes of the slice: x: 4, y: 4, z: 4 (z_hi: 2, z_lo: 2; z = z_hi * 2 + z_lo), core: 2. Of those that a mesh axis runs over, the one named last changes fastest.
Arguments:
- quantized: bfloat16 [524288, 1024], P(('region', 'tile')), may hold values from -6 to 6
- block_scales: float32 [8, 524288], P(None, ('region', 'tile')), may hold values from 0.25 to 4
- band_width: int32 [128], replicated, may hold values from 1 to 256, as said below
- valid_count: int32 [128], P(('region', 'tile')), may hold values from 1024 to 4096, as said below
- prior_basis: float32 [1024, 64], replicated, may hold values from -0.1875 to 0.1875
Outputs:
- projected: float32 [64, 524288], P(None, ('region', 'tile'))
- new_basis: float32 [1024, 64], replicated
The draws below stay inside these ranges and needn't reach their ends.
Inputs may be any that keep to these rules, and one draw needn't show every extreme that they name: `band_width`: some tile other than the first of its region has width 256 in every draw. `valid_count`: the last tile's count is 4096 in every draw.
All inputs are finite; a program needn't handle non-finite values.
Results may differ from the reference program's by a relative error of at most 0.0016.
Values may be sent and summed in bfloat16 or wider, within the bound.
No kernel may reach another device: no remote copies, remote signals or barrier semaphores. Data moves between devices by JAX's collectives and lax.ppermute only.
A program may use at most 128 MiB of HBM per device.

```python
import math
import jax
import jax.numpy as jnp
from jax import lax

D = 1024
K = 64
BLOCK = 128
BAND = 256
TOK_DEV = 4096
TILES = 128
TOKENS = 524288
NB = 8
N_REGION = 4
N_TILE = 32


def draw_quantized(key, part):
    noise_key, offset_key = jax.random.split(jax.random.fold_in(key, 101), 2)
    offsets = jax.random.normal(offset_key, (D,), jnp.float32) * 0.7
    ramp = 1.0 + 2.0 * jnp.arange(TOKENS, dtype=jnp.float32) / (TOKENS - 1)
    noise = jax.random.normal(noise_key, (TOKENS, D), jnp.float32)
    values = jnp.clip(noise + ramp[:, None] * offsets[None, :], -6.0, 6.0)
    return values.astype(jnp.bfloat16)


def draw_band_width(key, part):
    first_key, second_key, third_key = jax.random.split(jax.random.fold_in(key, 202), 3)
    widths = jax.random.randint(first_key, (TILES,), 1, BAND + 1)
    chosen = jax.random.randint(second_key, (), 0, N_REGION) * N_TILE + jax.random.randint(third_key, (), 1, N_TILE)
    return widths.at[chosen].set(BAND).astype(jnp.int32)


def draw_valid_count(key, part):
    jitter_key = jax.random.fold_in(key, 303)
    lowest = TOK_DEV // 3
    positions = jnp.arange(TILES, dtype=jnp.int32)
    baseline = lowest + positions * (TOK_DEV - lowest) // max(TILES - 1, 1)
    jitter = jax.random.randint(jitter_key, (TILES,), -(TOK_DEV // 8), TOK_DEV // 8 + 1)
    counts = jnp.clip(baseline + jitter, TOK_DEV // 4, TOK_DEV)
    return counts.at[TILES - 1].set(TOK_DEV).astype(jnp.int32)


def level_of(own_key, shape, cuts, least, top_value):
    gain, own = 1.0, jax.random.fold_in(own_key, 6)
    for dim, shards_of in cuts:
        heights = jnp.exp(jax.random.uniform(jax.random.fold_in(own, dim), (shards_of,), jnp.float32, least / len(cuts), top_value / len(cuts)))
        gain = gain * jnp.repeat(heights, shape[dim] // shards_of).reshape([-1 if axis == dim else 1 for axis in range(len(shape))])
    return gain


def gaussian(stream_key, dims, width, limit, held_as=jnp.bfloat16):
    array = jax.random.normal(stream_key, dims, jnp.float32) * width
    return jnp.minimum(jnp.maximum(array, -limit), limit).astype(held_as)


def setup_inputs(seed: int = 0) -> dict:
    key_of = jax.random.split(jax.random.key(seed), 6)
    quantized = draw_quantized(jax.random.fold_in(key_of[5], 71), 0)
    block_scales = jnp.clip(jnp.exp(math.log(4.0) - 2.7725887 * jax.random.uniform(key_of[1], (NB, TOKENS), jnp.float32) ** level_of(key_of[1], (NB, TOKENS), ((1, 128),), -0.2, 0.2)), 0.25, 4.0)
    band_width = draw_band_width(jax.random.fold_in(key_of[5], 71), 0)
    valid_count = draw_valid_count(jax.random.fold_in(key_of[5], 71), 0)
    prior_basis = gaussian(key_of[4], (D, K), D ** -0.5, 0.1875, jnp.float32)
    return dict(quantized=quantized, block_scales=block_scales, band_width=band_width, valid_count=valid_count, prior_basis=prior_basis)


def dequantize(quant_tile, scale_tile):
    blocks = quant_tile.astype(jnp.float32).reshape(TOK_DEV, D // BLOCK, BLOCK) * scale_tile.T[:, :, None]
    return blocks.reshape(TOK_DEV, D).astype(jnp.bfloat16)

def blend(initial, neighbour, chosen):
    summed = (initial.astype(jnp.float32) + neighbour.astype(jnp.float32)) * 0.5
    return jnp.where(chosen[:, None], summed, initial.astype(jnp.float32)).astype(jnp.bfloat16)

def reference(quantized, block_scales, band_width, valid_count, prior_basis):
    tile_count = N_REGION * N_TILE
    quant_tiles = quantized.reshape(tile_count, TOK_DEV, D)
    scale_tiles = block_scales.reshape(D // BLOCK, tile_count, TOK_DEV).transpose(1, 0, 2)
    restored = lax.map(lambda pieces: dequantize(pieces[0], pieces[1]), (quant_tiles, scale_tiles))
    position = jnp.arange(tile_count) % N_TILE
    left_width = jnp.where(position > 0, band_width, 0).astype(jnp.int32)
    right_width = jnp.where(position < N_TILE - 1, jnp.roll(band_width, -1), 0).astype(jnp.int32)
    head_rows = restored[:, :BAND]
    tail_rows = restored[:, TOK_DEV - BAND:]
    prev_tails = jnp.roll(tail_rows, 1, axis=0)
    next_heads = jnp.roll(head_rows, -1, axis=0)
    positions = jnp.arange(BAND)

    def edges(head_tile, tail_tile, prev_tail, next_head, lwidth, rwidth):
        blank = jnp.zeros((BAND, D), jnp.bfloat16)
        left_part = lax.dynamic_slice_in_dim(jnp.concatenate([prev_tail, blank], 0), (BAND - lwidth).astype(jnp.int32), BAND, 0)
        right_part = lax.dynamic_slice_in_dim(jnp.concatenate([blank, next_head], 0), rwidth.astype(jnp.int32), BAND, 0)
        return (blend(head_tile, left_part, positions < lwidth), blend(tail_tile, right_part, positions >= BAND - rwidth))
    new_heads, new_tails = jax.vmap(edges)(head_rows, tail_rows, prev_tails, next_heads, left_width, right_width)
    blended = restored.at[:, :BAND].set(new_heads).at[:, TOK_DEV - BAND:].set(new_tails)
    usable = jnp.arange(TOK_DEV)[None, :] < valid_count[:, None]
    masked = jnp.where(usable[:, :, None], blended, jnp.zeros((), jnp.bfloat16))

    def accumulate(running, tile_rows):
        products, feature_sums = running
        products = products + lax.dot_general(tile_rows.astype(jnp.float32), tile_rows.astype(jnp.float32), (((0,), (0,)), ((), ())), preferred_element_type=jnp.float32)
        feature_sums = feature_sums + jnp.sum(tile_rows.astype(jnp.float32), axis=0)
        return ((products, feature_sums), None)
    start_state = (jnp.zeros((D, D), jnp.float32), jnp.zeros((D,), jnp.float32))
    (products, feature_sums), _ = lax.scan(accumulate, start_state, masked)
    token_count = jnp.sum(valid_count.astype(jnp.float32))
    average = feature_sums / token_count
    gram = products - jnp.outer(feature_sums, average)
    update = jnp.dot(gram, prior_basis, precision=lax.Precision.HIGHEST)
    cross_sum = jnp.dot(update.T, update, precision=lax.Precision.HIGHEST)
    factor = jnp.linalg.cholesky(cross_sum)
    new_basis = jax.scipy.linalg.solve_triangular(factor, update.T, lower=True).T

    def project(pieces):
        tile_rows, usable_rows = pieces
        centred = jnp.where(usable_rows[:, None], tile_rows.astype(jnp.float32) - average, 0.0)
        return lax.dot_general(new_basis, centred, (((0,), (1,)), ((), ())), precision=lax.Precision.HIGHEST)
    projected = lax.map(project, (masked, usable))
    projected = projected.transpose(1, 0, 2).reshape(K, TOKENS)
    return (projected, new_basis)
```

```python
import functools

import jax
import jax.numpy as jnp
from jax import lax
from jax.experimental import pallas as pl
from jax.experimental.pallas import tpu as pltpu
from jax.sharding import PartitionSpec as P

BAND = 256
STEP = 512
ROWS = 72
AXES = ("region", "tile")
F32 = jnp.float32
BF16 = jnp.bfloat16
NT = (((1,), (1,)), ((), ()))
NN = (((1,), (0,)), ((), ()))


def split3(value):
    high = value.astype(BF16)
    rest = value - high.astype(F32)
    mid = rest.astype(BF16)
    low = (rest - mid.astype(F32)).astype(BF16)
    return high, mid, low


def dequantize(quant, scales):
    by_token = scales.T
    groups = scales.shape[0]
    width = quant.shape[1] // groups
    return [
        (quant[:, b * width : (b + 1) * width].astype(F32) * by_token[:, b : b + 1]).astype(BF16)
        for b in range(groups)
    ]


def reduced_rows(prior, tokens):
    keep = prior.shape[0] // 3
    wide = lax.dot_general(prior, tokens, NT, preferred_element_type=F32)
    return wide[:keep] + wide[keep : 2 * keep] + wide[2 * keep :]


def widths(width_ref, n_tile):
    tile = lax.axis_index("tile")
    number = lax.axis_index("region") * n_tile + tile
    left = jnp.where(tile > 0, width_ref[number], 0)
    last = width_ref.shape[0] - 1
    right = jnp.where(tile < n_tile - 1, width_ref[jnp.minimum(number + 1, last)], 0)
    return left, right


def band_kernel(valid_ref, head_ref, tail_ref, head_s_ref, tail_s_ref, prior_ref,
                forward_ref, backward_ref, prior3_ref, *, tok_rows):
    high, mid, low = split3(prior_ref[...].T)
    prior = jnp.concatenate([high, mid, low], 0)
    prior3_ref[...] = prior
    head = jnp.concatenate(dequantize(head_ref[...], head_s_ref[...]), 1)
    backward_ref[...] = reduced_rows(prior, head)
    tail = jnp.concatenate(dequantize(tail_ref[...], tail_s_ref[...]), 1)
    keep = prior.shape[0] // 3
    forward_ref[:keep, :] = reduced_rows(prior, tail)
    place = tok_rows - BAND + lax.broadcasted_iota(jnp.int32, (ROWS - keep, BAND), 1)
    forward_ref[keep:, :] = jnp.where(place < valid_ref[0], 2.0, 1.0)


def bulk_kernel(width_ref, valid_ref, quant_ref, scale_ref, prior3_ref,
                token_ref, sum_ref, *, tok_rows, n_tile):
    step = pl.program_id(0)
    left, right = widths(width_ref, n_tile)
    for b, block in enumerate(dequantize(quant_ref[...], scale_ref[...])):
        token_ref[:, b * block.shape[1] : (b + 1) * block.shape[1]] = block
    tokens = token_ref[...]
    reduced = reduced_rows(prior3_ref[...], tokens)
    place = step * STEP + lax.broadcasted_iota(jnp.int32, (1, STEP), 1)
    inner = (place >= left) & (place < tok_rows - right) & (place < valid_ref[0])
    weight = jnp.where(inner, 1.0, 0.0)
    reduced = reduced * weight
    high = reduced.astype(BF16)
    low = (reduced - high.astype(F32)).astype(BF16)
    extra = jnp.broadcast_to(weight, (16, STEP)).astype(BF16)
    part = lax.dot_general(jnp.concatenate([high, low, extra], 0), tokens, NN, preferred_element_type=F32)

    @pl.when(step == 0)
    def _():
        sum_ref[...] = part

    @pl.when(step > 0)
    def _():
        sum_ref[...] += part


def join_kernel(width_ref, valid_ref, head_ref, tail_ref, sum_ref, forward_ref, backward_ref,
                before_ref, after_ref, out_ref, *, tok_rows, n_tile):
    left, right = widths(width_ref, n_tile)
    keep = backward_ref.shape[0]
    place = lax.broadcasted_iota(jnp.int32, (1, BAND), 1)
    before = pltpu.roll(before_ref[...], lax.rem(left, BAND), 1)
    after = pltpu.roll(after_ref[...], lax.rem(BAND - right, BAND), 1)
    count = jnp.where(place < left, before[keep : keep + 1], 0.0)
    head = (backward_ref[...] + before[:keep]) * (count * 0.25)
    both = jnp.where(place >= BAND - right, forward_ref[keep : keep + 1, :], 0.0)
    tail = (forward_ref[:keep, :] + after) * (both * 0.25)
    total = sum_ref[...]
    for reduced, weight, rows in ((head, count, head_ref), (tail, both, tail_ref)):
        reduced = jnp.where(weight > 0.0, reduced, 0.0)
        high = reduced.astype(BF16)
        low = (reduced - high.astype(F32)).astype(BF16)
        extra = jnp.broadcast_to(weight * 0.5, (16, BAND)).astype(BF16)
        total = total + lax.dot_general(
            jnp.concatenate([high, low, extra], 0), rows[...], NN, preferred_element_type=F32
        )
    update = total[:keep] + total[keep : 2 * keep]
    row = lax.broadcasted_iota(jnp.int32, (ROWS - keep, total.shape[1]), 0)
    extra = jnp.where(row == 0, total[2 * keep : 2 * keep + ROWS - keep], valid_ref[0].astype(F32))
    for c in range(out_ref.shape[0]):
        out_ref[c, :keep, :] = update[:, c * 128 : (c + 1) * 128]
        out_ref[c, keep:, :] = extra[:, c * 128 : (c + 1) * 128]


def inverse_factor(square):
    size = square.shape[0]
    eye = (
        lax.broadcasted_iota(jnp.int32, (size, size), 0)
        == lax.broadcasted_iota(jnp.int32, (size, size), 1)
    ).astype(F32)
    both = jnp.concatenate([square, eye], 1)
    wide = (8, 2 * size)
    groups = size // 8
    rows = [both[8 * i : 8 * i + 8] for i in range(groups)]
    sublane = lax.broadcasted_iota(jnp.int32, wide, 0)
    done = []
    for j in range(groups):
        columns = [
            [jnp.broadcast_to(rows[i][:, 8 * j + k : 8 * j + k + 1], wide) for i in range(j, groups)]
            for k in range(8)
        ]
        scale = jnp.zeros(wide, F32)
        for k in range(8):
            pivot = jnp.broadcast_to(columns[k][0][k : k + 1], wide)
            scale = jnp.where(sublane == k, lax.rsqrt(pivot), scale)
            line = jnp.broadcast_to(rows[j][k : k + 1], wide) / pivot
            ratio = [
                jnp.broadcast_to(columns[k][0][m : m + 1], wide) / pivot for m in range(k + 1, 8)
            ]
            for i in range(j, groups):
                factor = columns[k][i - j]
                if i == j:
                    factor = jnp.where(sublane > k, factor, 0.0)
                rows[i] = rows[i] - factor * line
                for m in range(k + 1, 8):
                    columns[m][i - j] = columns[m][i - j] - factor * ratio[m - k - 1]
        done.append(rows[j] * scale)
    return jnp.concatenate(done, 0)[:, size:]


def basis_kernel(own_ref, other_ref, prior_ref, head_ref, tail_ref,
                 basis_ref, pair_ref, shift_ref, head_out_ref, tail_out_ref):
    core = lax.rem(lax.axis_index("region"), 2)
    y = lax.rem(lax.div(lax.axis_index("tile"), 2), 4)
    keep = prior_ref.shape[1]
    pieces = []
    for c in range(8):
        slot = jnp.bitwise_xor(c % 4, y)
        pieces.append(jnp.where(core == c // 4, own_ref[slot], other_ref[slot]))
    full = jnp.concatenate(pieces, 1)
    sums = full[keep : keep + 1]
    average = sums / full[keep + 1 : keep + 2]
    prior = prior_ref[...].T
    image = jnp.sum(prior * average, axis=1, keepdims=True)
    update = full[:keep] - image * sums
    square = lax.dot_general(update, update, NT, precision=lax.Precision.HIGHEST, preferred_element_type=F32)
    inverse = inverse_factor(square)
    basis = lax.dot_general(inverse, update, NN, precision=lax.Precision.HIGHEST, preferred_element_type=F32)
    basis_ref[...] = basis
    high = basis.astype(BF16)
    low = (basis - high.astype(F32)).astype(BF16)
    pair = jnp.concatenate([high, low], 0)
    pair_ref[...] = pair
    shift_ref[...] = jnp.broadcast_to(jnp.sum(basis * average, axis=1, keepdims=True), shift_ref.shape)
    for rows, out in ((head_ref, head_out_ref), (tail_ref, tail_out_ref)):
        wide = lax.dot_general(pair, rows[...], NT, preferred_element_type=F32)
        out[...] = wide[:keep] + wide[keep:]


def project_kernel(valid_ref, token_ref, pair_ref, shift_ref, basis_ref, out_ref, basis_out_ref):
    step = pl.program_id(0)
    keep = shift_ref.shape[0]
    wide = lax.dot_general(pair_ref[...], token_ref[...], NT, preferred_element_type=F32)
    place = step * STEP + lax.broadcasted_iota(jnp.int32, (1, STEP), 1)
    value = wide[:keep] + wide[keep:] - shift_ref[:, :1]
    out_ref[...] = jnp.where(place < valid_ref[0], value, 0.0)

    @pl.when(step == 0)
    def _():
        basis_out_ref[...] = basis_ref[...].T


def blend_kernel(width_ref, valid_ref, head_ref, tail_ref, before_ref, after_ref, shift_ref,
                 whole_ref, out_ref, buffer_ref, sem_ref, *, tok_rows, n_tile):
    left, right = widths(width_ref, n_tile)
    place = lax.broadcasted_iota(jnp.int32, (1, BAND), 1)
    shift = shift_ref[:, :1]
    before = pltpu.roll(before_ref[...], lax.rem(left, BAND), 1)
    after = pltpu.roll(after_ref[...], lax.rem(BAND - right, BAND), 1)
    head = jnp.where(place < left, (head_ref[...] + before) * 0.5, head_ref[...]) - shift
    tail = jnp.where(place >= BAND - right, (tail_ref[...] + after) * 0.5, tail_ref[...]) - shift
    start = tok_rows - BAND
    buffer_ref[0] = jnp.where(place < valid_ref[0], head, 0.0)
    buffer_ref[1] = jnp.where(start + place < valid_ref[0], tail, 0.0)
    first = pltpu.make_async_copy(buffer_ref.at[0], out_ref.at[:, pl.ds(0, BAND)], sem_ref.at[0])
    second = pltpu.make_async_copy(buffer_ref.at[1], out_ref.at[:, pl.ds(start, BAND)], sem_ref.at[1])
    first.start()
    second.start()
    first.wait()
    second.wait()


def smem():
    return pl.BlockSpec(memory_space=pltpu.SMEM)


def params(mib):
    return pltpu.CompilerParams(vmem_limit_bytes=mib << 20)


def flip(value, mask):
    pairs = [(g, g ^ mask) for g in range(128)]
    return lax.ppermute(value, AXES, pairs)


def pick(stack, index):
    return lax.dynamic_index_in_dim(stack, index, 0, keepdims=False)


def reduce_all(pieces):
    core = lax.axis_index("region") % 2
    y = (lax.axis_index("tile") // 2) % 4
    halves = pieces.reshape(2, 4, *pieces.shape[1:])
    half = pick(halves, core) + flip(pick(halves, 1 - core), 32)
    arrived = [flip(pick(half, y ^ k), k << 1) for k in range(1, 4)]
    mine = pick(half, y)
    for piece in arrived:
        mine = mine + piece
    arrived = [flip(mine, k << 3) for k in range(1, 4)]
    for piece in arrived:
        mine = mine + piece
    arrived = [flip(mine, mask) for mask in (1, 64, 65)]
    for piece in arrived:
        mine = mine + piece
    own = jnp.stack([mine] + [flip(mine, k << 1) for k in range(1, 4)])
    return own, flip(own, 32)


def per_device(quantized, block_scales, band_width, valid_count, prior_basis):
    tok_rows, feat_dim = quantized.shape
    keep = prior_basis.shape[1]
    groups = block_scales.shape[0]
    n_tile = lax.axis_size("tile")
    steps = tok_rows // STEP
    last = tok_rows // BAND - 1
    forward_pairs = [(i, i + 1) for i in range(n_tile - 1)]
    backward_pairs = [(i + 1, i) for i in range(n_tile - 1)]
    head_rows = pl.BlockSpec((BAND, feat_dim), lambda i: (0, 0))
    tail_rows = pl.BlockSpec((BAND, feat_dim), lambda i: (last, 0))

    def whole(*shape):
        return pl.BlockSpec(shape, lambda i: (0,) * len(shape))

    forward, backward, prior3 = pl.pallas_call(
        functools.partial(band_kernel, tok_rows=tok_rows),
        grid=(1,),
        in_specs=[
            smem(),
            head_rows,
            tail_rows,
            pl.BlockSpec((groups, BAND), lambda i: (0, 0)),
            pl.BlockSpec((groups, BAND), lambda i: (0, last)),
            whole(feat_dim, keep),
        ],
        out_specs=[whole(ROWS, BAND), whole(keep, BAND), whole(3 * keep, feat_dim)],
        out_shape=[
            jax.ShapeDtypeStruct((ROWS, BAND), F32),
            jax.ShapeDtypeStruct((keep, BAND), F32),
            jax.ShapeDtypeStruct((3 * keep, feat_dim), BF16),
        ],
        compiler_params=params(24),
        name="band",
    )(valid_count, quantized, quantized, block_scales, block_scales, prior_basis)
    before = lax.ppermute(forward, "tile", forward_pairs)
    after = lax.ppermute(backward, "tile", backward_pairs)
    tokens, sums = pl.pallas_call(
        functools.partial(bulk_kernel, tok_rows=tok_rows, n_tile=n_tile),
        grid=(steps,),
        in_specs=[
            smem(),
            smem(),
            pl.BlockSpec((STEP, feat_dim), lambda i: (i, 0)),
            pl.BlockSpec((groups, STEP), lambda i: (0, i)),
            whole(3 * keep, feat_dim),
        ],
        out_specs=[pl.BlockSpec((STEP, feat_dim), lambda i: (i, 0)), whole(2 * keep + 16, feat_dim)],
        out_shape=[
            jax.ShapeDtypeStruct((tok_rows, feat_dim), BF16),
            jax.ShapeDtypeStruct((2 * keep + 16, feat_dim), F32),
        ],
        compiler_params=params(32),
        name="bulk",
    )(band_width, valid_count, quantized, block_scales, prior3)
    pieces = pl.pallas_call(
        functools.partial(join_kernel, tok_rows=tok_rows, n_tile=n_tile),
        grid=(1,),
        in_specs=[
            smem(),
            smem(),
            head_rows,
            tail_rows,
            whole(2 * keep + 16, feat_dim),
            whole(ROWS, BAND),
            whole(keep, BAND),
            whole(ROWS, BAND),
            whole(keep, BAND),
        ],
        out_specs=whole(feat_dim // 128, ROWS, 128),
        out_shape=jax.ShapeDtypeStruct((feat_dim // 128, ROWS, 128), F32),
        compiler_params=params(24),
        name="join",
    )(band_width, valid_count, tokens, tokens, sums, forward, backward, before, after)
    own, other = reduce_all(pieces)
    basis, pair, shift, head, tail = pl.pallas_call(
        basis_kernel,
        grid=(1,),
        in_specs=[whole(4, ROWS, 128), whole(4, ROWS, 128), whole(feat_dim, keep), head_rows, tail_rows],
        out_specs=[
            whole(keep, feat_dim),
            whole(2 * keep, feat_dim),
            whole(keep, 128),
            whole(keep, BAND),
            whole(keep, BAND),
        ],
        out_shape=[
            jax.ShapeDtypeStruct((keep, feat_dim), F32),
            jax.ShapeDtypeStruct((2 * keep, feat_dim), BF16),
            jax.ShapeDtypeStruct((keep, 128), F32),
            jax.ShapeDtypeStruct((keep, BAND), F32),
            jax.ShapeDtypeStruct((keep, BAND), F32),
        ],
        compiler_params=params(24),
        name="basis",
    )(own, other, prior_basis, tokens, tokens)
    before = lax.ppermute(tail, "tile", forward_pairs)
    after = lax.ppermute(head, "tile", backward_pairs)
    raw, new_basis = pl.pallas_call(
        project_kernel,
        grid=(steps,),
        in_specs=[
            smem(),
            pl.BlockSpec((STEP, feat_dim), lambda i: (i, 0)),
            whole(2 * keep, feat_dim),
            whole(keep, 128),
            whole(keep, feat_dim),
        ],
        out_specs=[pl.BlockSpec((keep, STEP), lambda i: (0, i)), whole(feat_dim, keep)],
        out_shape=[
            jax.ShapeDtypeStruct((keep, tok_rows), F32),
            jax.ShapeDtypeStruct((feat_dim, keep), F32),
        ],
        compiler_params=params(24),
        name="project",
    )(valid_count, tokens, pair, shift, basis)
    projected = pl.pallas_call(
        functools.partial(blend_kernel, tok_rows=tok_rows, n_tile=n_tile),
        in_specs=[smem(), smem()]
        + [pl.BlockSpec(memory_space=pltpu.VMEM)] * 5
        + [pl.BlockSpec(memory_space=pl.ANY)],
        out_specs=pl.BlockSpec(memory_space=pl.ANY),
        out_shape=jax.ShapeDtypeStruct((keep, tok_rows), F32),
        scratch_shapes=[pltpu.VMEM((2, keep, BAND), F32), pltpu.SemaphoreType.DMA((2,))],
        input_output_aliases={7: 0},
        compiler_params=params(8),
        name="blend",
    )(band_width, valid_count, head, tail, before, after, shift, raw)
    return projected, new_basis


def solution(mesh):
    return jax.shard_map(
        per_device,
        mesh=mesh,
        in_specs=(
            P(("region", "tile"), None),
            P(None, ("region", "tile")),
            P(),
            P(("region", "tile")),
            P(),
        ),
        out_specs=(P(None, ("region", "tile")), P()),
        check_vma=False,
    )
```

```python
import functools

import jax
import jax.numpy as jnp
from jax import lax
from jax.experimental import pallas as pl
from jax.experimental.pallas import tpu as pltpu
from jax.sharding import PartitionSpec as P

BAND = 256
STEP = 512
ROWS = 72
AXES = ("region", "tile")
F32 = jnp.float32
BF16 = jnp.bfloat16
NT = (((1,), (1,)), ((), ()))
NN = (((1,), (0,)), ((), ()))


def split3(value):
    high = value.astype(BF16)
    rest = value - high.astype(F32)
    mid = rest.astype(BF16)
    low = (rest - mid.astype(F32)).astype(BF16)
    return high, mid, low


def dequantize(quant, scales):
    by_token = scales.T
    groups = scales.shape[0]
    width = quant.shape[1] // groups
    return [
        (quant[:, b * width : (b + 1) * width].astype(F32) * by_token[:, b : b + 1]).astype(BF16)
        for b in range(groups)
    ]


def reduced_rows(prior, tokens):
    wide = lax.dot_general(tokens, prior, NN, preferred_element_type=F32)
    half = (wide[:, :128] + wide[:, 128:]).T
    return half[:64] + half[64:]


def widths(width_ref, n_tile):
    tile = lax.axis_index("tile")
    number = lax.axis_index("region") * n_tile + tile
    left = jnp.where(tile > 0, width_ref[number], 0)
    last = width_ref.shape[0] - 1
    right = jnp.where(tile < n_tile - 1, width_ref[jnp.minimum(number + 1, last)], 0)
    return left, right


def band_kernel(valid_ref, head_ref, tail_ref, head_s_ref, tail_s_ref, prior_ref,
                forward_ref, backward_ref, prior3_ref, head_out_ref, tail_out_ref, *, tok_rows):
    high, mid, low = split3(prior_ref[...])
    prior = jnp.concatenate([high, mid, low, jnp.zeros_like(low)], 0).T
    prior3_ref[...] = prior
    head = jnp.concatenate(dequantize(head_ref[...], head_s_ref[...]), 1)
    head_out_ref[...] = head
    backward_ref[...] = reduced_rows(prior, head)
    tail = jnp.concatenate(dequantize(tail_ref[...], tail_s_ref[...]), 1)
    tail_out_ref[...] = tail
    keep = high.shape[0]
    forward_ref[:keep, :] = reduced_rows(prior, tail)
    place = tok_rows - BAND + lax.broadcasted_iota(jnp.int32, (ROWS - keep, BAND), 1)
    forward_ref[keep:, :] = jnp.where(place < valid_ref[0], 2.0, 1.0)


def bulk_kernel(width_ref, valid_ref, quant_ref, scale_ref, prior3_ref,
                token_ref, sum_ref, *, tok_rows, n_tile):
    step = pl.program_id(0)
    left, right = widths(width_ref, n_tile)
    for b, block in enumerate(dequantize(quant_ref[...], scale_ref[...])):
        token_ref[:, b * block.shape[1] : (b + 1) * block.shape[1]] = block
    tokens = token_ref[...]
    reduced = reduced_rows(prior3_ref[...], tokens)
    place = step * STEP + lax.broadcasted_iota(jnp.int32, (1, STEP), 1)
    inner = (place >= left) & (place < tok_rows - right) & (place < valid_ref[0])
    weight = jnp.where(inner, 1.0, 0.0)
    reduced = reduced * weight
    high = reduced.astype(BF16)
    low = (reduced - high.astype(F32)).astype(BF16)
    extra = jnp.broadcast_to(weight, (16, STEP)).astype(BF16)
    part = lax.dot_general(jnp.concatenate([high, low, extra], 0), tokens, NN, preferred_element_type=F32)

    @pl.when(step == 0)
    def _():
        sum_ref[...] = part

    @pl.when(step > 0)
    def _():
        sum_ref[...] += part


def join_kernel(width_ref, valid_ref, head_ref, tail_ref, sum_ref, forward_ref, backward_ref,
                before_ref, after_ref, out_ref, *, tok_rows, n_tile):
    left, right = widths(width_ref, n_tile)
    keep = backward_ref.shape[0]
    place = lax.broadcasted_iota(jnp.int32, (1, BAND), 1)
    before = pltpu.roll(before_ref[...], lax.rem(left, BAND), 1)
    after = pltpu.roll(after_ref[...], lax.rem(BAND - right, BAND), 1)
    count = jnp.where(place < left, before[keep : keep + 1], 0.0)
    head = (backward_ref[...] + before[:keep]) * (count * 0.25)
    both = jnp.where(place >= BAND - right, forward_ref[keep : keep + 1, :], 0.0)
    tail = (forward_ref[:keep, :] + after) * (both * 0.25)
    total = sum_ref[...]
    for reduced, weight, rows in ((head, count, head_ref), (tail, both, tail_ref)):
        reduced = jnp.where(weight > 0.0, reduced, 0.0)
        high = reduced.astype(BF16)
        low = (reduced - high.astype(F32)).astype(BF16)
        extra = jnp.broadcast_to(weight * 0.5, (16, BAND)).astype(BF16)
        total = total + lax.dot_general(
            jnp.concatenate([high, low, extra], 0), rows[...], NN, preferred_element_type=F32
        )
    update = total[:keep] + total[keep : 2 * keep]
    row = lax.broadcasted_iota(jnp.int32, (ROWS - keep, total.shape[1]), 0)
    extra = jnp.where(row == 0, total[2 * keep : 2 * keep + ROWS - keep], valid_ref[0].astype(F32))
    for c in range(out_ref.shape[0]):
        out_ref[c, :keep, :] = update[:, c * 128 : (c + 1) * 128]
        out_ref[c, keep:, :] = extra[:, c * 128 : (c + 1) * 128]


def inverse_factor(square):
    size = square.shape[0]
    eye = (
        lax.broadcasted_iota(jnp.int32, (size, size), 0)
        == lax.broadcasted_iota(jnp.int32, (size, size), 1)
    ).astype(F32)
    both = jnp.concatenate([square, eye], 1)
    wide = (8, 2 * size)
    groups = size // 8
    rows = [both[8 * i : 8 * i + 8] for i in range(groups)]
    sublane = lax.broadcasted_iota(jnp.int32, wide, 0)
    done = []
    for j in range(groups):
        columns = [
            [jnp.broadcast_to(rows[i][:, 8 * j + k : 8 * j + k + 1], wide) for i in range(j, groups)]
            for k in range(8)
        ]
        scale = jnp.zeros(wide, F32)
        for k in range(8):
            pivot = jnp.broadcast_to(columns[k][0][k : k + 1], wide)
            scale = jnp.where(sublane == k, lax.rsqrt(pivot), scale)
            line = jnp.broadcast_to(rows[j][k : k + 1], wide) / pivot
            ratio = [
                jnp.broadcast_to(columns[k][0][m : m + 1], wide) / pivot for m in range(k + 1, 8)
            ]
            for i in range(j, groups):
                factor = columns[k][i - j]
                if i == j:
                    factor = jnp.where(sublane > k, factor, 0.0)
                rows[i] = rows[i] - factor * line
                for m in range(k + 1, 8):
                    columns[m][i - j] = columns[m][i - j] - factor * ratio[m - k - 1]
        done.append(rows[j] * scale)
    return jnp.concatenate(done, 0)[:, size:]


def basis_kernel(own_ref, other_ref, prior_ref, head_ref, tail_ref,
                 basis_ref, pair_ref, shift_ref, head_out_ref, tail_out_ref):
    core = lax.rem(lax.axis_index("region"), 2)
    y = lax.rem(lax.div(lax.axis_index("tile"), 2), 4)
    keep = prior_ref.shape[0]
    pieces = []
    for c in range(8):
        slot = jnp.bitwise_xor(c % 4, y)
        pieces.append(jnp.where(core == c // 4, own_ref[slot], other_ref[slot]))
    full = jnp.concatenate(pieces, 1)
    sums = full[keep : keep + 1]
    average = sums / full[keep + 1 : keep + 2]
    image = jnp.sum(prior_ref[...] * average, axis=1, keepdims=True)
    update = full[:keep] - image * sums
    square = lax.dot_general(update, update, NT, precision=lax.Precision.HIGHEST, preferred_element_type=F32)
    inverse = inverse_factor(square)
    basis = lax.dot_general(inverse, update, NN, precision=lax.Precision.HIGHEST, preferred_element_type=F32)
    basis_ref[...] = basis
    high = basis.astype(BF16)
    low = (basis - high.astype(F32)).astype(BF16)
    pair = jnp.concatenate([high, low], 0).T
    pair_ref[...] = pair
    shift_ref[...] = jnp.broadcast_to(jnp.sum(basis * average, axis=1, keepdims=True), shift_ref.shape)
    for rows, out in ((head_ref, head_out_ref), (tail_ref, tail_out_ref)):
        wide = lax.dot_general(rows[...], pair, NN, preferred_element_type=F32).T
        out[...] = wide[:keep] + wide[keep:]


def project_kernel(valid_ref, token_ref, pair_ref, shift_ref, out_ref):
    step = pl.program_id(0)
    keep = shift_ref.shape[0]
    wide = lax.dot_general(token_ref[...], pair_ref[...], NN, preferred_element_type=F32).T
    place = step * STEP + lax.broadcasted_iota(jnp.int32, (1, STEP), 1)
    value = wide[:keep] + wide[keep:] - shift_ref[:, :1]
    out_ref[...] = jnp.where(place < valid_ref[0], value, 0.0)


def blend_kernel(width_ref, valid_ref, head_ref, tail_ref, before_ref, after_ref, shift_ref,
                 whole_ref, out_ref, buffer_ref, sem_ref, *, tok_rows, n_tile):
    left, right = widths(width_ref, n_tile)
    place = lax.broadcasted_iota(jnp.int32, (1, BAND), 1)
    shift = shift_ref[:, :1]
    before = pltpu.roll(before_ref[...], lax.rem(left, BAND), 1)
    after = pltpu.roll(after_ref[...], lax.rem(BAND - right, BAND), 1)
    head = jnp.where(place < left, (head_ref[...] + before) * 0.5, head_ref[...]) - shift
    tail = jnp.where(place >= BAND - right, (tail_ref[...] + after) * 0.5, tail_ref[...]) - shift
    start = tok_rows - BAND
    buffer_ref[0] = jnp.where(place < valid_ref[0], head, 0.0)
    buffer_ref[1] = jnp.where(start + place < valid_ref[0], tail, 0.0)
    first = pltpu.make_async_copy(buffer_ref.at[0], out_ref.at[:, pl.ds(0, BAND)], sem_ref.at[0])
    second = pltpu.make_async_copy(buffer_ref.at[1], out_ref.at[:, pl.ds(start, BAND)], sem_ref.at[1])
    first.start()
    second.start()
    first.wait()
    second.wait()


def smem():
    return pl.BlockSpec(memory_space=pltpu.SMEM)


def params(mib):
    return pltpu.CompilerParams(vmem_limit_bytes=mib << 20)


def flip(value, mask):
    pairs = [(g, g ^ mask) for g in range(128)]
    return lax.ppermute(value, AXES, pairs)


def pick(stack, index):
    return lax.dynamic_index_in_dim(stack, index, 0, keepdims=False)


def reduce_all(pieces):
    core = lax.axis_index("region") % 2
    y = (lax.axis_index("tile") // 2) % 4
    halves = pieces.reshape(2, 4, *pieces.shape[1:])
    half = pick(halves, core) + flip(pick(halves, 1 - core), 32)
    arrived = [flip(pick(half, y ^ k), k << 1) for k in range(1, 4)]
    mine = pick(half, y)
    for piece in arrived:
        mine = mine + piece
    arrived = [flip(mine, k << 3) for k in range(1, 4)]
    for piece in arrived:
        mine = mine + piece
    arrived = [flip(mine, mask) for mask in (1, 64, 65)]
    for piece in arrived:
        mine = mine + piece
    own = jnp.stack([mine] + [flip(mine, k << 1) for k in range(1, 4)])
    return own, flip(own, 32)


def per_device(quantized, block_scales, band_width, valid_count, prior_basis):
    tok_rows, feat_dim = quantized.shape
    keep = prior_basis.shape[1]
    groups = block_scales.shape[0]
    n_tile = lax.axis_size("tile")
    steps = tok_rows // STEP
    last = tok_rows // BAND - 1
    forward_pairs = [(i, i + 1) for i in range(n_tile - 1)]
    backward_pairs = [(i + 1, i) for i in range(n_tile - 1)]
    head_rows = pl.BlockSpec((BAND, feat_dim), lambda i: (0, 0))
    tail_rows = pl.BlockSpec((BAND, feat_dim), lambda i: (last, 0))

    def whole(*shape):
        return pl.BlockSpec(shape, lambda i: (0,) * len(shape))

    quantized = pltpu.with_memory_space_constraint(quantized, pltpu.HBM)
    prior = prior_basis.T
    forward, backward, prior3, head_tokens, tail_tokens = pl.pallas_call(
        functools.partial(band_kernel, tok_rows=tok_rows),
        grid=(1,),
        in_specs=[
            smem(),
            head_rows,
            tail_rows,
            pl.BlockSpec((groups, BAND), lambda i: (0, 0)),
            pl.BlockSpec((groups, BAND), lambda i: (0, last)),
            whole(keep, feat_dim),
        ],
        out_specs=[
            whole(ROWS, BAND),
            whole(keep, BAND),
            whole(feat_dim, 4 * keep),
            whole(BAND, feat_dim),
            whole(BAND, feat_dim),
        ],
        out_shape=[
            jax.ShapeDtypeStruct((ROWS, BAND), F32),
            jax.ShapeDtypeStruct((keep, BAND), F32),
            jax.ShapeDtypeStruct((feat_dim, 4 * keep), BF16),
            jax.ShapeDtypeStruct((BAND, feat_dim), BF16),
            jax.ShapeDtypeStruct((BAND, feat_dim), BF16),
        ],
        compiler_params=params(24),
        name="band",
    )(valid_count, quantized, quantized, block_scales, block_scales, prior)
    before = lax.ppermute(forward, "tile", forward_pairs)
    after = lax.ppermute(backward, "tile", backward_pairs)
    tokens, sums = pl.pallas_call(
        functools.partial(bulk_kernel, tok_rows=tok_rows, n_tile=n_tile),
        grid=(steps,),
        in_specs=[
            smem(),
            smem(),
            pl.BlockSpec((STEP, feat_dim), lambda i: (i, 0)),
            pl.BlockSpec((groups, STEP), lambda i: (0, i)),
            whole(feat_dim, 4 * keep),
        ],
        out_specs=[pl.BlockSpec((STEP, feat_dim), lambda i: (i, 0)), whole(2 * keep + 16, feat_dim)],
        out_shape=[
            pltpu.HBM((tok_rows, feat_dim), BF16),
            jax.ShapeDtypeStruct((2 * keep + 16, feat_dim), F32),
        ],
        compiler_params=params(32),
        name="bulk",
    )(band_width, valid_count, quantized, block_scales, prior3)
    pieces = pl.pallas_call(
        functools.partial(join_kernel, tok_rows=tok_rows, n_tile=n_tile),
        grid=(1,),
        in_specs=[
            smem(),
            smem(),
            whole(BAND, feat_dim),
            whole(BAND, feat_dim),
            whole(2 * keep + 16, feat_dim),
            whole(ROWS, BAND),
            whole(keep, BAND),
            whole(ROWS, BAND),
            whole(keep, BAND),
        ],
        out_specs=whole(feat_dim // 128, ROWS, 128),
        out_shape=jax.ShapeDtypeStruct((feat_dim // 128, ROWS, 128), F32),
        compiler_params=params(24),
        name="join",
    )(band_width, valid_count, head_tokens, tail_tokens, sums, forward, backward, before, after)
    own, other = reduce_all(pieces)
    basis, pair, shift, head, tail = pl.pallas_call(
        basis_kernel,
        grid=(1,),
        in_specs=[
            whole(4, ROWS, 128),
            whole(4, ROWS, 128),
            whole(keep, feat_dim),
            whole(BAND, feat_dim),
            whole(BAND, feat_dim),
        ],
        out_specs=[
            whole(keep, feat_dim),
            whole(feat_dim, 2 * keep),
            whole(keep, 128),
            whole(keep, BAND),
            whole(keep, BAND),
        ],
        out_shape=[
            jax.ShapeDtypeStruct((keep, feat_dim), F32),
            jax.ShapeDtypeStruct((feat_dim, 2 * keep), BF16),
            jax.ShapeDtypeStruct((keep, 128), F32),
            jax.ShapeDtypeStruct((keep, BAND), F32),
            jax.ShapeDtypeStruct((keep, BAND), F32),
        ],
        compiler_params=params(24),
        name="basis",
    )(own, other, prior, head_tokens, tail_tokens)
    before = lax.ppermute(tail, "tile", forward_pairs)
    after = lax.ppermute(head, "tile", backward_pairs)
    raw = pl.pallas_call(
        project_kernel,
        grid=(steps,),
        in_specs=[
            smem(),
            pl.BlockSpec((STEP, feat_dim), lambda i: (i, 0)),
            whole(feat_dim, 2 * keep),
            whole(keep, 128),
        ],
        out_specs=pl.BlockSpec((keep, STEP), lambda i: (0, i)),
        out_shape=jax.ShapeDtypeStruct((keep, tok_rows), F32),
        compiler_params=params(24),
        name="project",
    )(valid_count, pltpu.with_memory_space_constraint(tokens, pltpu.HBM), pair, shift)
    projected = pl.pallas_call(
        functools.partial(blend_kernel, tok_rows=tok_rows, n_tile=n_tile),
        in_specs=[smem(), smem()]
        + [pl.BlockSpec(memory_space=pltpu.VMEM)] * 5
        + [pl.BlockSpec(memory_space=pl.ANY)],
        out_specs=pl.BlockSpec(memory_space=pl.ANY),
        out_shape=jax.ShapeDtypeStruct((keep, tok_rows), F32),
        scratch_shapes=[pltpu.VMEM((2, keep, BAND), F32), pltpu.SemaphoreType.DMA((2,))],
        input_output_aliases={7: 0},
        compiler_params=params(8),
        name="blend",
    )(band_width, valid_count, head, tail, before, after, shift, raw)
    return projected, basis.T


def solution(mesh):
    return jax.shard_map(
        per_device,
        mesh=mesh,
        in_specs=(
            P(("region", "tile"), None),
            P(None, ("region", "tile")),
            P(),
            P(("region", "tile")),
            P(),
        ),
        out_specs=(P(None, ("region", "tile")), P()),
        check_vma=False,
    )
```

```python
import functools

import jax
import jax.numpy as jnp
from jax import lax
from jax.experimental import pallas as pl
from jax.experimental.pallas import tpu as pltpu
from jax.sharding import PartitionSpec as P


BAND = 256
STEP = 1024
ROWS = 72
AXES = ("region", "tile")
F32 = jnp.float32
BF16 = jnp.bfloat16
NT = (((1,), (1,)), ((), ()))
NN = (((1,), (0,)), ((), ()))


def split3(value):
    high = value.astype(BF16)
    rest = value - high.astype(F32)
    mid = rest.astype(BF16)
    low = (rest - mid.astype(F32)).astype(BF16)
    return high, mid, low


def dequantize(quant, scales):
    rows = quant.shape[0]
    groups = scales.shape[0]
    width = quant.shape[1] // groups
    return [
        (
            quant[:, b * width : (b + 1) * width].astype(F32)
            * jnp.broadcast_to(scales[b : b + 1], (width, rows)).T
        ).astype(BF16)
        for b in range(groups)
    ]


def reduced_rows(prior, tokens):
    wide = lax.dot_general(tokens, prior, NN, preferred_element_type=F32)
    half = (wide[:, :128] + wide[:, 128:]).T
    return half[:64] + half[64:]


def widths(width_ref, n_tile):
    tile = lax.axis_index("tile")
    number = lax.axis_index("region") * n_tile + tile
    left = jnp.where(tile > 0, width_ref[number], 0)
    last = width_ref.shape[0] - 1
    right = jnp.where(tile < n_tile - 1, width_ref[jnp.minimum(number + 1, last)], 0)
    return left, right


def band_kernel(valid_ref, head_ref, tail_ref, head_s_ref, tail_s_ref, prior_ref,
                forward_ref, backward_ref, prior3_ref, head_out_ref, tail_out_ref, *, tok_rows):
    high, mid, low = split3(prior_ref[...])
    prior = jnp.concatenate([high, mid, low, jnp.zeros_like(low)], 0).T
    prior3_ref[...] = prior
    head = jnp.concatenate(dequantize(head_ref[...], head_s_ref[...]), 1)
    head_out_ref[...] = head
    backward_ref[...] = reduced_rows(prior, head)
    tail = jnp.concatenate(dequantize(tail_ref[...], tail_s_ref[...]), 1)
    tail_out_ref[...] = tail
    keep = high.shape[0]
    forward_ref[:keep, :] = reduced_rows(prior, tail)
    place = tok_rows - BAND + lax.broadcasted_iota(jnp.int32, (ROWS - keep, BAND), 1)
    forward_ref[keep:, :] = jnp.where(place < valid_ref[0], 2.0, 1.0)


def bulk_kernel(width_ref, valid_ref, quant_ref, scale_ref, prior3_ref,
                token_ref, sum_ref, raw_ref, held_ref, in_sem, out_sem, *, tok_rows, n_tile):
    steps = tok_rows // STEP
    chunks = [pl.ds(step * STEP, STEP) for step in range(steps)]
    arrive = [
        pltpu.make_async_copy(quant_ref.at[rows], raw_ref.at[rows], in_sem.at[step])
        for step, rows in enumerate(chunks)
    ]
    leave = [
        pltpu.make_async_copy(held_ref.at[rows], token_ref.at[rows], out_sem.at[step])
        for step, rows in enumerate(chunks)
    ]
    for copy in arrive:
        copy.start()
    left, right = widths(width_ref, n_tile)
    for step in range(steps + 1):
        if step < steps:
            arrive[step].wait()
            blocks = dequantize(raw_ref[chunks[step], :], scale_ref[:, chunks[step]])
            for b, block in enumerate(blocks):
                held_ref[chunks[step], b * block.shape[1] : (b + 1) * block.shape[1]] = block
        if step > 0:
            tokens = held_ref[chunks[step - 1], :]
            reduced = reduced_rows(prior3_ref[...], tokens)
            place = (step - 1) * STEP + lax.broadcasted_iota(jnp.int32, (1, STEP), 1)
            inner = (place >= left) & (place < tok_rows - right) & (place < valid_ref[0])
            weight = jnp.where(inner, 1.0, 0.0)
            reduced = reduced * weight
            high = reduced.astype(BF16)
            low = (reduced - high.astype(F32)).astype(BF16)
            extra = jnp.broadcast_to(weight, (16, STEP)).astype(BF16)
            part = lax.dot_general(
                jnp.concatenate([high, low, extra], 0), tokens, NN, preferred_element_type=F32
            )
            sum_ref[...] = part if step == 1 else sum_ref[...] + part
            leave[step - 1].start()
    for copy in leave:
        copy.wait()


def join_kernel(width_ref, valid_ref, head_ref, tail_ref, sum_ref, forward_ref, backward_ref,
                before_ref, after_ref, out_ref, *, tok_rows, n_tile):
    left, right = widths(width_ref, n_tile)
    keep = backward_ref.shape[0]
    place = lax.broadcasted_iota(jnp.int32, (1, BAND), 1)
    before = pltpu.roll(before_ref[...], lax.rem(left, BAND), 1)
    after = pltpu.roll(after_ref[...], lax.rem(BAND - right, BAND), 1)
    count = jnp.where(place < left, before[keep : keep + 1], 0.0)
    head = (backward_ref[...] + before[:keep]) * (count * 0.25)
    both = jnp.where(place >= BAND - right, forward_ref[keep : keep + 1, :], 0.0)
    tail = (forward_ref[:keep, :] + after) * (both * 0.25)
    total = sum_ref[...]
    for reduced, weight, rows in ((head, count, head_ref), (tail, both, tail_ref)):
        reduced = jnp.where(weight > 0.0, reduced, 0.0)
        high = reduced.astype(BF16)
        low = (reduced - high.astype(F32)).astype(BF16)
        extra = jnp.broadcast_to(weight * 0.5, (16, BAND)).astype(BF16)
        total = total + lax.dot_general(
            jnp.concatenate([high, low, extra], 0), rows[...], NN, preferred_element_type=F32
        )
    update = total[:keep] + total[keep : 2 * keep]
    row = lax.broadcasted_iota(jnp.int32, (ROWS - keep, total.shape[1]), 0)
    extra = jnp.where(row == 0, total[2 * keep : 2 * keep + ROWS - keep], valid_ref[0].astype(F32))
    for c in range(out_ref.shape[0]):
        out_ref[c, :keep, :] = update[:, c * 128 : (c + 1) * 128]
        out_ref[c, keep:, :] = extra[:, c * 128 : (c + 1) * 128]


def inverse_factor(square):
    size = square.shape[0]
    eye = (
        lax.broadcasted_iota(jnp.int32, (size, size), 0)
        == lax.broadcasted_iota(jnp.int32, (size, size), 1)
    ).astype(F32)
    both = jnp.concatenate([square, eye], 1)
    wide = (8, 2 * size)
    groups = size // 8
    rows = [both[8 * i : 8 * i + 8] for i in range(groups)]
    sublane = lax.broadcasted_iota(jnp.int32, wide, 0)
    done = []
    for j in range(groups):
        columns = [
            [jnp.broadcast_to(rows[i][:, 8 * j + k : 8 * j + k + 1], wide) for i in range(j, groups)]
            for k in range(8)
        ]
        scale = jnp.zeros(wide, F32)
        for k in range(8):
            pivot = jnp.broadcast_to(columns[k][0][k : k + 1], wide)
            scale = jnp.where(sublane == k, lax.rsqrt(pivot), scale)
            line = jnp.broadcast_to(rows[j][k : k + 1], wide) / pivot
            ratio = [
                jnp.broadcast_to(columns[k][0][m : m + 1], wide) / pivot for m in range(k + 1, 8)
            ]
            for i in range(j, groups):
                factor = columns[k][i - j]
                if i == j:
                    factor = jnp.where(sublane > k, factor, 0.0)
                rows[i] = rows[i] - factor * line
                for m in range(k + 1, 8):
                    columns[m][i - j] = columns[m][i - j] - factor * ratio[m - k - 1]
        done.append(rows[j] * scale)
    return jnp.concatenate(done, 0)[:, size:]


def finish_kernel(width_ref, valid_ref, own_ref, other_ref, prior_ref, before_ref, after_ref, token_ref,
                  basis_ref, out_ref, held_ref, value_ref, in_sem, out_sem, *, tok_rows, n_tile):
    steps = tok_rows // STEP
    chunks = [pl.ds(step * STEP, STEP) for step in range(steps)]
    arrive = [
        pltpu.make_async_copy(token_ref.at[rows], held_ref.at[rows], in_sem.at[step])
        for step, rows in enumerate(chunks)
    ]
    leave = [
        pltpu.make_async_copy(value_ref.at[:, rows], out_ref.at[:, rows], out_sem.at[step])
        for step, rows in enumerate(chunks)
    ]
    for copy in arrive:
        copy.start()
    left, right = widths(width_ref, n_tile)
    core = lax.rem(lax.axis_index("region"), 2)
    y = lax.rem(lax.div(lax.axis_index("tile"), 2), 4)
    keep = prior_ref.shape[0]
    pieces = []
    for c in range(8):
        slot = jnp.bitwise_xor(c % 4, y)
        pieces.append(jnp.where(core == c // 4, own_ref[slot], other_ref[slot]))
    full = jnp.concatenate(pieces, 1)
    sums = full[keep : keep + 1]
    average = sums / full[keep + 1 : keep + 2]
    image = jnp.sum(prior_ref[...] * average, axis=1, keepdims=True)
    update = full[:keep] - image * sums
    square = lax.dot_general(update, update, NT, precision=lax.Precision.HIGHEST, preferred_element_type=F32)
    inverse = inverse_factor(square)
    basis = lax.dot_general(inverse, update, NN, precision=lax.Precision.HIGHEST, preferred_element_type=F32)
    basis_ref[...] = basis
    high = basis.astype(BF16)
    low = (basis - high.astype(F32)).astype(BF16)
    pair = jnp.concatenate([high, low], 0).T
    shift = jnp.sum(basis * average, axis=1, keepdims=True)

    def project(rows):
        wide = lax.dot_general(rows, pair, NN, preferred_element_type=F32).T
        return wide[:keep] + wide[keep:]

    before = pltpu.roll(project(before_ref[...]), lax.rem(left, BAND), 1)
    after = pltpu.roll(project(after_ref[...]), lax.rem(BAND - right, BAND), 1)
    near = lax.broadcasted_iota(jnp.int32, (1, BAND), 1)
    for step in range(steps):
        arrive[step].wait()
        value = project(held_ref[chunks[step], :])
        if step == 0:
            head = jnp.where(near < left, (value[:, :BAND] + before) * 0.5, value[:, :BAND])
            value = jnp.concatenate([head, value[:, BAND:]], 1)
        if step == steps - 1:
            edge = STEP - BAND
            tail = jnp.where(near >= BAND - right, (value[:, edge:] + after) * 0.5, value[:, edge:])
            value = jnp.concatenate([value[:, :edge], tail], 1)
        place = step * STEP + lax.broadcasted_iota(jnp.int32, (1, STEP), 1)
        value_ref[:, chunks[step]] = jnp.where(place < valid_ref[0], value - shift, 0.0)
        if step > 0:
            leave[step - 1].start()
    leave[steps - 1].start()
    for copy in leave:
        copy.wait()


def smem():
    return pl.BlockSpec(memory_space=pltpu.SMEM)


def near():
    return pl.BlockSpec(memory_space=pltpu.VMEM)


def far():
    return pl.BlockSpec(memory_space=pltpu.HBM)


def params(mib):
    return pltpu.CompilerParams(vmem_limit_bytes=mib << 20)


def flip(value, mask):
    pairs = [(g, g ^ mask) for g in range(128)]
    return lax.ppermute(value, AXES, pairs)


def pick(stack, index):
    return lax.dynamic_index_in_dim(stack, index, 0, keepdims=False)


def reduce_all(pieces):
    core = lax.axis_index("region") % 2
    y = (lax.axis_index("tile") // 2) % 4
    halves = pieces.reshape(2, 4, *pieces.shape[1:])
    half = pick(halves, core) + flip(pick(halves, 1 - core), 32)
    arrived = [flip(pick(half, y ^ k), k << 1) for k in range(1, 4)]
    mine = pick(half, y)
    for piece in arrived:
        mine = mine + piece
    arrived = [flip(mine, k << 3) for k in range(1, 4)]
    for piece in arrived:
        mine = mine + piece
    arrived = [flip(mine, mask) for mask in (1, 64, 65)]
    for piece in arrived:
        mine = mine + piece
    own = jnp.stack([mine] + [flip(mine, k << 1) for k in range(1, 4)])
    return own, flip(own, 32)


def per_device(quantized, block_scales, band_width, valid_count, prior_basis):
    tok_rows, feat_dim = quantized.shape
    keep = prior_basis.shape[1]
    groups = block_scales.shape[0]
    n_tile = lax.axis_size("tile")
    steps = tok_rows // STEP
    last = tok_rows // BAND - 1
    forward_pairs = [(i, i + 1) for i in range(n_tile - 1)]
    backward_pairs = [(i + 1, i) for i in range(n_tile - 1)]
    head_rows = pl.BlockSpec((BAND, feat_dim), lambda i: (0, 0))
    tail_rows = pl.BlockSpec((BAND, feat_dim), lambda i: (last, 0))

    def whole(*shape):
        return pl.BlockSpec(shape, lambda i: (0,) * len(shape))

    quantized = pltpu.with_memory_space_constraint(quantized, pltpu.HBM)
    prior = prior_basis.T
    prior_far = pltpu.with_memory_space_constraint(prior, pltpu.HBM)
    scales_far = pltpu.with_memory_space_constraint(block_scales, pltpu.HBM)
    forward, backward, prior3, head_tokens, tail_tokens = pl.pallas_call(
        functools.partial(band_kernel, tok_rows=tok_rows),
        grid=(1,),
        in_specs=[
            smem(),
            head_rows,
            tail_rows,
            pl.BlockSpec((groups, BAND), lambda i: (0, 0)),
            pl.BlockSpec((groups, BAND), lambda i: (0, last)),
            whole(keep, feat_dim),
        ],
        out_specs=[
            whole(ROWS, BAND),
            whole(keep, BAND),
            whole(feat_dim, 4 * keep),
            whole(BAND, feat_dim),
            whole(BAND, feat_dim),
        ],
        out_shape=[
            jax.ShapeDtypeStruct((ROWS, BAND), F32),
            jax.ShapeDtypeStruct((keep, BAND), F32),
            jax.ShapeDtypeStruct((feat_dim, 4 * keep), BF16),
            jax.ShapeDtypeStruct((BAND, feat_dim), BF16),
            jax.ShapeDtypeStruct((BAND, feat_dim), BF16),
        ],
        compiler_params=params(24),
        name="band",
    )(valid_count, quantized, quantized, scales_far, scales_far, prior_far)
    before = lax.ppermute(forward, "tile", forward_pairs)
    after = lax.ppermute(backward, "tile", backward_pairs)
    before_rows = lax.ppermute(tail_tokens, "tile", forward_pairs)
    after_rows = lax.ppermute(head_tokens, "tile", backward_pairs)
    bulk = pl.pallas_call(
        functools.partial(bulk_kernel, tok_rows=tok_rows, n_tile=n_tile),
        in_specs=[smem(), smem(), far(), near(), near()],
        out_specs=[far(), near()],
        out_shape=[
            pltpu.HBM((tok_rows, feat_dim), BF16),
            jax.ShapeDtypeStruct((2 * keep + 16, feat_dim), F32),
        ],
        scratch_shapes=[
            pltpu.VMEM((tok_rows, feat_dim), BF16),
            pltpu.VMEM((tok_rows, feat_dim), BF16),
            pltpu.SemaphoreType.DMA((steps,)),
            pltpu.SemaphoreType.DMA((steps,)),
        ],
        compiler_params=params(40),
        name="bulk",
    )
    tokens, sums = bulk(band_width, valid_count, quantized, block_scales, prior3)
    pieces = pl.pallas_call(
        functools.partial(join_kernel, tok_rows=tok_rows, n_tile=n_tile),
        grid=(1,),
        in_specs=[
            smem(),
            smem(),
            whole(BAND, feat_dim),
            whole(BAND, feat_dim),
            whole(2 * keep + 16, feat_dim),
            whole(ROWS, BAND),
            whole(keep, BAND),
            whole(ROWS, BAND),
            whole(keep, BAND),
        ],
        out_specs=whole(feat_dim // 128, ROWS, 128),
        out_shape=jax.ShapeDtypeStruct((feat_dim // 128, ROWS, 128), F32),
        compiler_params=params(24),
        name="join",
    )(band_width, valid_count, head_tokens, tail_tokens, sums, forward, backward, before, after)
    own, other = reduce_all(pieces)
    basis, projected = pl.pallas_call(
        functools.partial(finish_kernel, tok_rows=tok_rows, n_tile=n_tile),
        in_specs=[smem(), smem()] + [near()] * 5 + [far()],
        out_specs=[near(), far()],
        out_shape=[
            jax.ShapeDtypeStruct((keep, feat_dim), F32),
            pltpu.HBM((keep, tok_rows), F32),
        ],
        scratch_shapes=[
            pltpu.VMEM((tok_rows, feat_dim), BF16),
            pltpu.VMEM((keep, tok_rows), F32),
            pltpu.SemaphoreType.DMA((steps,)),
            pltpu.SemaphoreType.DMA((steps,)),
        ],
        compiler_params=params(32),
        name="finish",
    )(
        band_width,
        valid_count,
        own,
        other,
        prior,
        before_rows,
        after_rows,
        pltpu.with_memory_space_constraint(tokens, pltpu.HBM),
    )
    return projected, basis.T


def solution(mesh):
    return jax.shard_map(
        per_device,
        mesh=mesh,
        in_specs=(
            P(("region", "tile"), None),
            P(None, ("region", "tile")),
            P(),
            P(("region", "tile")),
            P(),
        ),
        out_specs=(P(None, ("region", "tile")), P()),
        check_vma=False,
    )
```

```python
import functools

import jax
import jax.numpy as jnp
from jax import lax
from jax.experimental import pallas as pl
from jax.experimental.pallas import tpu as pltpu
from jax.sharding import PartitionSpec as P


BAND = 256
STEP = 1024
ROWS = 72
AXES = ("region", "tile")
F32 = jnp.float32
BF16 = jnp.bfloat16
NT = (((1,), (1,)), ((), ()))
NN = (((1,), (0,)), ((), ()))


def split3(value):
    high = value.astype(BF16)
    rest = value - high.astype(F32)
    mid = rest.astype(BF16)
    low = (rest - mid.astype(F32)).astype(BF16)
    return high, mid, low


def dequantize(quant, scales):
    rows = quant.shape[0]
    groups = scales.shape[0]
    width = quant.shape[1] // groups
    return [
        (
            quant[:, b * width : (b + 1) * width].astype(F32)
            * jnp.broadcast_to(scales[b : b + 1], (width, rows)).T
        ).astype(BF16)
        for b in range(groups)
    ]


def reduced_rows(prior, tokens):
    wide = lax.dot_general(tokens, prior, NN, preferred_element_type=F32)
    half = (wide[:, :128] + wide[:, 128:]).T
    return half[:64] + half[64:]


def widths(width_ref, n_tile):
    tile = lax.axis_index("tile")
    number = lax.axis_index("region") * n_tile + tile
    left = jnp.where(tile > 0, width_ref[number], 0)
    last = width_ref.shape[0] - 1
    right = jnp.where(tile < n_tile - 1, width_ref[jnp.minimum(number + 1, last)], 0)
    return left, right


def band_kernel(valid_ref, head_ref, tail_ref, head_s_ref, tail_s_ref, prior_ref,
                forward_ref, backward_ref, prior3_ref, head_out_ref, tail_out_ref, *, tok_rows):
    high, mid, low = split3(prior_ref[...])
    prior = jnp.concatenate([high, mid, low, jnp.zeros_like(low)], 0).T
    prior3_ref[...] = prior
    head = jnp.concatenate(dequantize(head_ref[...], head_s_ref[...]), 1)
    head_out_ref[...] = head
    backward_ref[...] = reduced_rows(prior, head)
    tail = jnp.concatenate(dequantize(tail_ref[...], tail_s_ref[...]), 1)
    tail_out_ref[...] = tail
    keep = high.shape[0]
    forward_ref[:keep, :] = reduced_rows(prior, tail)
    place = tok_rows - BAND + lax.broadcasted_iota(jnp.int32, (ROWS - keep, BAND), 1)
    forward_ref[keep:, :] = jnp.where(place < valid_ref[0], 2.0, 1.0)


def bulk_kernel(width_ref, valid_ref, quant_ref, scale_ref, prior3_ref,
                token_ref, sum_ref, raw_ref, held_ref, in_sem, out_sem, *, tok_rows, n_tile):
    steps = tok_rows // STEP
    chunks = [pl.ds(step * STEP, STEP) for step in range(steps)]
    arrive = [
        pltpu.make_async_copy(quant_ref.at[rows], raw_ref.at[rows], in_sem.at[step])
        for step, rows in enumerate(chunks)
    ]
    leave = [
        pltpu.make_async_copy(held_ref.at[rows], token_ref.at[rows], out_sem.at[step])
        for step, rows in enumerate(chunks)
    ]
    for copy in arrive:
        copy.start()
    left, right = widths(width_ref, n_tile)
    for step in range(steps + 1):
        if step < steps:
            arrive[step].wait()
            blocks = dequantize(raw_ref[chunks[step], :], scale_ref[:, chunks[step]])
            for b, block in enumerate(blocks):
                held_ref[chunks[step], b * block.shape[1] : (b + 1) * block.shape[1]] = block
        if step > 0:
            tokens = held_ref[chunks[step - 1], :]
            reduced = reduced_rows(prior3_ref[...], tokens)
            place = (step - 1) * STEP + lax.broadcasted_iota(jnp.int32, (1, STEP), 1)
            inner = (place >= left) & (place < tok_rows - right) & (place < valid_ref[0])
            weight = jnp.where(inner, 1.0, 0.0)
            reduced = reduced * weight
            high = reduced.astype(BF16)
            low = (reduced - high.astype(F32)).astype(BF16)
            extra = jnp.broadcast_to(weight, (16, STEP)).astype(BF16)
            part = lax.dot_general(
                jnp.concatenate([high, low, extra], 0), tokens, NN, preferred_element_type=F32
            )
            sum_ref[...] = part if step == 1 else sum_ref[...] + part
            leave[step - 1].start()
    for copy in leave:
        copy.wait()


def join_kernel(width_ref, valid_ref, head_ref, tail_ref, sum_ref, forward_ref, backward_ref,
                before_ref, after_ref, out_ref, *, tok_rows, n_tile):
    left, right = widths(width_ref, n_tile)
    keep = backward_ref.shape[0]
    place = lax.broadcasted_iota(jnp.int32, (1, BAND), 1)
    before = pltpu.roll(before_ref[...], lax.rem(left, BAND), 1)
    after = pltpu.roll(after_ref[...], lax.rem(BAND - right, BAND), 1)
    count = jnp.where(place < left, before[keep : keep + 1], 0.0)
    head = (backward_ref[...] + before[:keep]) * (count * 0.25)
    both = jnp.where(place >= BAND - right, forward_ref[keep : keep + 1, :], 0.0)
    tail = (forward_ref[:keep, :] + after) * (both * 0.25)
    total = sum_ref[...]
    for reduced, weight, rows in ((head, count, head_ref), (tail, both, tail_ref)):
        reduced = jnp.where(weight > 0.0, reduced, 0.0)
        high = reduced.astype(BF16)
        low = (reduced - high.astype(F32)).astype(BF16)
        extra = jnp.broadcast_to(weight * 0.5, (16, BAND)).astype(BF16)
        total = total + lax.dot_general(
            jnp.concatenate([high, low, extra], 0), rows[...], NN, preferred_element_type=F32
        )
    update = total[:keep] + total[keep : 2 * keep]
    row = lax.broadcasted_iota(jnp.int32, (ROWS - keep, total.shape[1]), 0)
    extra = jnp.where(row == 0, total[2 * keep : 2 * keep + ROWS - keep], valid_ref[0].astype(F32))
    for c in range(out_ref.shape[0]):
        out_ref[c, :keep, :] = update[:, c * 128 : (c + 1) * 128]
        out_ref[c, keep:, :] = extra[:, c * 128 : (c + 1) * 128]


def inverse_factor(square):
    size = square.shape[0]
    eye = (
        lax.broadcasted_iota(jnp.int32, (size, size), 0)
        == lax.broadcasted_iota(jnp.int32, (size, size), 1)
    ).astype(F32)
    both = jnp.concatenate([square, eye], 1)
    wide = (8, 2 * size)
    groups = size // 8
    rows = [both[8 * i : 8 * i + 8] for i in range(groups)]
    sublane = lax.broadcasted_iota(jnp.int32, wide, 0)
    done = []
    for j in range(groups):
        columns = [
            [jnp.broadcast_to(rows[i][:, 8 * j + k : 8 * j + k + 1], wide) for i in range(j, groups)]
            for k in range(8)
        ]
        scale = jnp.zeros(wide, F32)
        for k in range(8):
            pivot = jnp.broadcast_to(columns[k][0][k : k + 1], wide)
            scale = jnp.where(sublane == k, lax.rsqrt(pivot), scale)
            line = jnp.broadcast_to(rows[j][k : k + 1], wide) / pivot
            ratio = [
                jnp.broadcast_to(columns[k][0][m : m + 1], wide) / pivot for m in range(k + 1, 8)
            ]
            for i in range(j, groups):
                factor = columns[k][i - j]
                if i == j:
                    factor = jnp.where(sublane > k, factor, 0.0)
                rows[i] = rows[i] - factor * line
                for m in range(k + 1, 8):
                    columns[m][i - j] = columns[m][i - j] - factor * ratio[m - k - 1]
        done.append(rows[j] * scale)
    return jnp.concatenate(done, 0)[:, size:]


def basis_kernel(own_ref, other_ref, prior_ref, head_ref, tail_ref, far_ref,
                 basis_ref, pair_ref, shift_ref, head_out_ref, tail_out_ref, token_ref, sem):
    size = token_ref.shape[0] // sem.shape[0]
    arrive = [
        pltpu.make_async_copy(far_ref.at[pl.ds(i * size, size)], token_ref.at[pl.ds(i * size, size)], sem.at[i])
        for i in range(sem.shape[0])
    ]
    for copy in arrive:
        copy.start()
    core = lax.rem(lax.axis_index("region"), 2)
    y = lax.rem(lax.div(lax.axis_index("tile"), 2), 4)
    keep = prior_ref.shape[0]
    pieces = []
    for c in range(8):
        slot = jnp.bitwise_xor(c % 4, y)
        pieces.append(jnp.where(core == c // 4, own_ref[slot], other_ref[slot]))
    full = jnp.concatenate(pieces, 1)
    sums = full[keep : keep + 1]
    average = sums / full[keep + 1 : keep + 2]
    image = jnp.sum(prior_ref[...] * average, axis=1, keepdims=True)
    update = full[:keep] - image * sums
    square = lax.dot_general(update, update, NT, precision=lax.Precision.HIGHEST, preferred_element_type=F32)
    inverse = inverse_factor(square)
    basis = lax.dot_general(inverse, update, NN, precision=lax.Precision.HIGHEST, preferred_element_type=F32)
    basis_ref[...] = basis
    high = basis.astype(BF16)
    low = (basis - high.astype(F32)).astype(BF16)
    pair = jnp.concatenate([high, low], 0).T
    pair_ref[...] = pair
    shift_ref[...] = jnp.broadcast_to(jnp.sum(basis * average, axis=1, keepdims=True), shift_ref.shape)
    for rows, out in ((head_ref, head_out_ref), (tail_ref, tail_out_ref)):
        wide = lax.dot_general(rows[...], pair, NN, preferred_element_type=F32).T
        out[...] = wide[:keep] + wide[keep:]
    for copy in arrive:
        copy.wait()


def project_kernel(valid_ref, token_ref, pair_ref, shift_ref, out_ref, value_ref, out_sem, *, tok_rows):
    keep = shift_ref.shape[0]
    steps = tok_rows // STEP
    leave = []
    for step in range(steps):
        rows = pl.ds(step * STEP, STEP)
        wide = lax.dot_general(token_ref[rows, :], pair_ref[...], NN, preferred_element_type=F32).T
        place = step * STEP + lax.broadcasted_iota(jnp.int32, (1, STEP), 1)
        value = wide[:keep] + wide[keep:] - shift_ref[:, :1]
        value_ref[:, rows] = jnp.where(place < valid_ref[0], value, 0.0)
        leave.append(pltpu.make_async_copy(value_ref.at[:, rows], out_ref.at[:, rows], out_sem.at[step]))
        if step > 0:
            leave[step - 1].start()
    leave[steps - 1].start()
    for copy in leave:
        copy.wait()


def blend_kernel(width_ref, valid_ref, head_ref, tail_ref, before_ref, after_ref, shift_ref,
                 whole_ref, out_ref, buffer_ref, sem_ref, *, tok_rows, n_tile):
    left, right = widths(width_ref, n_tile)
    place = lax.broadcasted_iota(jnp.int32, (1, BAND), 1)
    shift = shift_ref[:, :1]
    before = pltpu.roll(before_ref[...], lax.rem(left, BAND), 1)
    after = pltpu.roll(after_ref[...], lax.rem(BAND - right, BAND), 1)
    head = jnp.where(place < left, (head_ref[...] + before) * 0.5, head_ref[...]) - shift
    tail = jnp.where(place >= BAND - right, (tail_ref[...] + after) * 0.5, tail_ref[...]) - shift
    start = tok_rows - BAND
    buffer_ref[0] = jnp.where(place < valid_ref[0], head, 0.0)
    buffer_ref[1] = jnp.where(start + place < valid_ref[0], tail, 0.0)
    first = pltpu.make_async_copy(buffer_ref.at[0], out_ref.at[:, pl.ds(0, BAND)], sem_ref.at[0])
    second = pltpu.make_async_copy(buffer_ref.at[1], out_ref.at[:, pl.ds(start, BAND)], sem_ref.at[1])
    first.start()
    second.start()
    first.wait()
    second.wait()


def smem():
    return pl.BlockSpec(memory_space=pltpu.SMEM)


def near():
    return pl.BlockSpec(memory_space=pltpu.VMEM)


def far():
    return pl.BlockSpec(memory_space=pltpu.HBM)


def params(mib):
    return pltpu.CompilerParams(vmem_limit_bytes=mib << 20)


def flip(value, mask):
    pairs = [(g, g ^ mask) for g in range(128)]
    return lax.ppermute(value, AXES, pairs)


def pick(stack, index):
    return lax.dynamic_index_in_dim(stack, index, 0, keepdims=False)


def reduce_all(pieces):
    core = lax.axis_index("region") % 2
    y = (lax.axis_index("tile") // 2) % 4
    halves = pieces.reshape(2, 4, *pieces.shape[1:])
    half = pick(halves, core) + flip(pick(halves, 1 - core), 32)
    arrived = [flip(pick(half, y ^ k), k << 1) for k in range(1, 4)]
    mine = pick(half, y)
    for piece in arrived:
        mine = mine + piece
    arrived = [flip(mine, k << 3) for k in range(1, 4)]
    for piece in arrived:
        mine = mine + piece
    arrived = [flip(mine, mask) for mask in (1, 64, 65)]
    for piece in arrived:
        mine = mine + piece
    own = jnp.stack([mine] + [flip(mine, k << 1) for k in range(1, 4)])
    return own, flip(own, 32)


def per_device(quantized, block_scales, band_width, valid_count, prior_basis):
    tok_rows, feat_dim = quantized.shape
    keep = prior_basis.shape[1]
    groups = block_scales.shape[0]
    n_tile = lax.axis_size("tile")
    steps = tok_rows // STEP
    last = tok_rows // BAND - 1
    forward_pairs = [(i, i + 1) for i in range(n_tile - 1)]
    backward_pairs = [(i + 1, i) for i in range(n_tile - 1)]
    head_rows = pl.BlockSpec((BAND, feat_dim), lambda i: (0, 0))
    tail_rows = pl.BlockSpec((BAND, feat_dim), lambda i: (last, 0))

    def whole(*shape):
        return pl.BlockSpec(shape, lambda i: (0,) * len(shape))

    quant_far = pltpu.with_memory_space_constraint(quantized, pltpu.HBM)
    prior = prior_basis.T
    prior_far = pltpu.with_memory_space_constraint(prior, pltpu.HBM)
    scales_far = pltpu.with_memory_space_constraint(block_scales, pltpu.HBM)
    forward, backward, prior3, head_tokens, tail_tokens = pl.pallas_call(
        functools.partial(band_kernel, tok_rows=tok_rows),
        grid=(1,),
        in_specs=[
            smem(),
            head_rows,
            tail_rows,
            pl.BlockSpec((groups, BAND), lambda i: (0, 0)),
            pl.BlockSpec((groups, BAND), lambda i: (0, last)),
            whole(keep, feat_dim),
        ],
        out_specs=[
            whole(ROWS, BAND),
            whole(keep, BAND),
            whole(feat_dim, 4 * keep),
            whole(BAND, feat_dim),
            whole(BAND, feat_dim),
        ],
        out_shape=[
            jax.ShapeDtypeStruct((ROWS, BAND), F32),
            jax.ShapeDtypeStruct((keep, BAND), F32),
            jax.ShapeDtypeStruct((feat_dim, 4 * keep), BF16),
            jax.ShapeDtypeStruct((BAND, feat_dim), BF16),
            jax.ShapeDtypeStruct((BAND, feat_dim), BF16),
        ],
        compiler_params=params(24),
        name="band",
    )(valid_count, quant_far, quant_far, scales_far, scales_far, prior_far)
    before = lax.ppermute(forward, "tile", forward_pairs)
    after = lax.ppermute(backward, "tile", backward_pairs)
    bulk = pl.pallas_call(
        functools.partial(bulk_kernel, tok_rows=tok_rows, n_tile=n_tile),
        in_specs=[smem(), smem(), far(), near(), near()],
        out_specs=[far(), near()],
        out_shape=[
            pltpu.HBM((tok_rows, feat_dim), BF16),
            jax.ShapeDtypeStruct((2 * keep + 16, feat_dim), F32),
        ],
        scratch_shapes=[
            pltpu.VMEM((tok_rows, feat_dim), BF16),
            pltpu.VMEM((tok_rows, feat_dim), BF16),
            pltpu.SemaphoreType.DMA((steps,)),
            pltpu.SemaphoreType.DMA((steps,)),
        ],
        compiler_params=params(32),
        name="bulk",
    )
    tokens, sums = bulk(band_width, valid_count, quant_far, block_scales, prior3)
    pieces = pl.pallas_call(
        functools.partial(join_kernel, tok_rows=tok_rows, n_tile=n_tile),
        grid=(1,),
        in_specs=[
            smem(),
            smem(),
            whole(BAND, feat_dim),
            whole(BAND, feat_dim),
            whole(2 * keep + 16, feat_dim),
            whole(ROWS, BAND),
            whole(keep, BAND),
            whole(ROWS, BAND),
            whole(keep, BAND),
        ],
        out_specs=whole(feat_dim // 128, ROWS, 128),
        out_shape=jax.ShapeDtypeStruct((feat_dim // 128, ROWS, 128), F32),
        compiler_params=params(24),
        name="join",
    )(band_width, valid_count, head_tokens, tail_tokens, sums, forward, backward, before, after)
    own, other = reduce_all(pieces)
    basis, pair, shift, head, tail, tokens = pl.pallas_call(
        basis_kernel,
        in_specs=[near()] * 5 + [far()],
        out_specs=[near()] * 6,
        out_shape=[
            jax.ShapeDtypeStruct((keep, feat_dim), F32),
            jax.ShapeDtypeStruct((feat_dim, 2 * keep), BF16),
            jax.ShapeDtypeStruct((keep, 128), F32),
            jax.ShapeDtypeStruct((keep, BAND), F32),
            jax.ShapeDtypeStruct((keep, BAND), F32),
            jax.ShapeDtypeStruct((tok_rows, feat_dim), BF16),
        ],
        scratch_shapes=[pltpu.SemaphoreType.DMA((8,))],
        compiler_params=params(24),
        name="basis",
    )(own, other, prior, head_tokens, tail_tokens, pltpu.with_memory_space_constraint(tokens, pltpu.HBM))
    before = lax.ppermute(tail, "tile", forward_pairs)
    after = lax.ppermute(head, "tile", backward_pairs)
    raw = pl.pallas_call(
        functools.partial(project_kernel, tok_rows=tok_rows),
        in_specs=[smem(), near(), near(), near()],
        out_specs=far(),
        out_shape=pltpu.HBM((keep, tok_rows), F32),
        scratch_shapes=[pltpu.VMEM((keep, tok_rows), F32), pltpu.SemaphoreType.DMA((steps,))],
        compiler_params=params(20),
        name="project",
    )(valid_count, tokens, pair, shift)
    projected = pl.pallas_call(
        functools.partial(blend_kernel, tok_rows=tok_rows, n_tile=n_tile),
        in_specs=[smem(), smem()]
        + [pl.BlockSpec(memory_space=pltpu.VMEM)] * 5
        + [pl.BlockSpec(memory_space=pl.ANY)],
        out_specs=pl.BlockSpec(memory_space=pl.ANY),
        out_shape=jax.ShapeDtypeStruct((keep, tok_rows), F32),
        scratch_shapes=[pltpu.VMEM((2, keep, BAND), F32), pltpu.SemaphoreType.DMA((2,))],
        input_output_aliases={7: 0},
        compiler_params=params(8),
        name="blend",
    )(band_width, valid_count, head, tail, before, after, shift, raw)
    return projected, basis.T


def solution(mesh):
    return jax.shard_map(
        per_device,
        mesh=mesh,
        in_specs=(
            P(("region", "tile"), None),
            P(None, ("region", "tile")),
            P(),
            P(("region", "tile")),
            P(),
        ),
        out_specs=(P(None, ("region", "tile")), P()),
        check_vma=False,
    )
```

```python
import functools

import jax
import jax.numpy as jnp
from jax import lax
from jax.experimental import pallas as pl
from jax.experimental.pallas import tpu as pltpu
from jax.sharding import PartitionSpec as P


BAND = 256
STEP = 1024
ROWS = 72
AXES = ("region", "tile")
F32 = jnp.float32
BF16 = jnp.bfloat16
NT = (((1,), (1,)), ((), ()))
NN = (((1,), (0,)), ((), ()))


def split3(value):
    high = value.astype(BF16)
    rest = value - high.astype(F32)
    mid = rest.astype(BF16)
    low = (rest - mid.astype(F32)).astype(BF16)
    return high, mid, low


def dequantize(quant, scales):
    rows = quant.shape[0]
    groups = scales.shape[0]
    width = quant.shape[1] // groups
    return [
        (
            quant[:, b * width : (b + 1) * width].astype(F32)
            * jnp.broadcast_to(scales[b : b + 1], (width, rows)).T
        ).astype(BF16)
        for b in range(groups)
    ]


def reduced_rows(prior, tokens):
    wide = lax.dot_general(tokens, prior, NN, preferred_element_type=F32)
    half = (wide[:, :128] + wide[:, 128:]).T
    return half[:64] + half[64:]


def begin(fetch, count):
    def one(i, carry):
        fetch(i).start()
        return carry

    lax.fori_loop(0, count, one, 0)


def widths(width_ref, n_tile):
    tile = lax.axis_index("tile")
    number = lax.axis_index("region") * n_tile + tile
    left = jnp.where(tile > 0, width_ref[number], 0)
    last = width_ref.shape[0] - 1
    right = jnp.where(tile < n_tile - 1, width_ref[jnp.minimum(number + 1, last)], 0)
    return left, right


def band_kernel(valid_ref, head_ref, tail_ref, head_s_ref, tail_s_ref, prior_ref,
                forward_ref, backward_ref, prior3_ref, head_out_ref, tail_out_ref, *, tok_rows):
    high, mid, low = split3(prior_ref[...])
    prior = jnp.concatenate([high, mid, low, jnp.zeros_like(low)], 0).T
    prior3_ref[...] = prior
    head = jnp.concatenate(dequantize(head_ref[...], head_s_ref[...]), 1)
    head_out_ref[...] = head
    backward_ref[...] = reduced_rows(prior, head)
    tail = jnp.concatenate(dequantize(tail_ref[...], tail_s_ref[...]), 1)
    tail_out_ref[...] = tail
    keep = high.shape[0]
    forward_ref[:keep, :] = reduced_rows(prior, tail)
    place = tok_rows - BAND + lax.broadcasted_iota(jnp.int32, (ROWS - keep, BAND), 1)
    forward_ref[keep:, :] = jnp.where(place < valid_ref[0], 2.0, 1.0)


def bulk_kernel(width_ref, valid_ref, quant_ref, scale_ref, prior3_ref,
                token_ref, sum_ref, raw_ref, held_ref, in_sem, out_sem, *, tok_rows, n_tile):
    steps = tok_rows // STEP
    chunks = [pl.ds(step * STEP, STEP) for step in range(steps)]

    def fetch(i):
        rows = pl.ds(pl.multiple_of(i * STEP, STEP), STEP)
        return pltpu.make_async_copy(quant_ref.at[rows], raw_ref.at[rows], in_sem.at[i])

    begin(fetch, steps)
    leave = [
        pltpu.make_async_copy(held_ref.at[rows], token_ref.at[rows], out_sem.at[step])
        for step, rows in enumerate(chunks)
    ]
    left, right = widths(width_ref, n_tile)
    for step in range(steps + 1):
        if step < steps:
            fetch(step).wait()
            blocks = dequantize(raw_ref[chunks[step], :], scale_ref[:, chunks[step]])
            for b, block in enumerate(blocks):
                held_ref[chunks[step], b * block.shape[1] : (b + 1) * block.shape[1]] = block
        if step > 0:
            tokens = held_ref[chunks[step - 1], :]
            reduced = reduced_rows(prior3_ref[...], tokens)
            place = (step - 1) * STEP + lax.broadcasted_iota(jnp.int32, (1, STEP), 1)
            inner = (place >= left) & (place < tok_rows - right) & (place < valid_ref[0])
            weight = jnp.where(inner, 1.0, 0.0)
            reduced = reduced * weight
            high = reduced.astype(BF16)
            low = (reduced - high.astype(F32)).astype(BF16)
            extra = jnp.broadcast_to(weight, (16, STEP)).astype(BF16)
            part = lax.dot_general(
                jnp.concatenate([high, low, extra], 0), tokens, NN, preferred_element_type=F32
            )
            sum_ref[...] = part if step == 1 else sum_ref[...] + part
            leave[step - 1].start()
    for copy in leave:
        copy.wait()


def join_kernel(width_ref, valid_ref, head_ref, tail_ref, sum_ref, forward_ref, backward_ref,
                before_ref, after_ref, out_ref, *, tok_rows, n_tile):
    left, right = widths(width_ref, n_tile)
    keep = backward_ref.shape[0]
    place = lax.broadcasted_iota(jnp.int32, (1, BAND), 1)
    before = pltpu.roll(before_ref[...], lax.rem(left, BAND), 1)
    after = pltpu.roll(after_ref[...], lax.rem(BAND - right, BAND), 1)
    count = jnp.where(place < left, before[keep : keep + 1], 0.0)
    head = (backward_ref[...] + before[:keep]) * (count * 0.25)
    both = jnp.where(place >= BAND - right, forward_ref[keep : keep + 1, :], 0.0)
    tail = (forward_ref[:keep, :] + after) * (both * 0.25)
    total = sum_ref[...]
    for reduced, weight, rows in ((head, count, head_ref), (tail, both, tail_ref)):
        reduced = jnp.where(weight > 0.0, reduced, 0.0)
        high = reduced.astype(BF16)
        low = (reduced - high.astype(F32)).astype(BF16)
        extra = jnp.broadcast_to(weight * 0.5, (16, BAND)).astype(BF16)
        total = total + lax.dot_general(
            jnp.concatenate([high, low, extra], 0), rows[...], NN, preferred_element_type=F32
        )
    update = total[:keep] + total[keep : 2 * keep]
    row = lax.broadcasted_iota(jnp.int32, (8, 128), 0)
    parts = out_ref.shape[0]
    share = total.shape[1] // 128 // parts
    for part in range(parts):
        extra = jnp.where(row == share, valid_ref[0].astype(F32), 0.0)
        for c in range(share):
            lanes = slice((part * share + c) * 128, (part * share + c + 1) * 128)
            out_ref[part, c * keep : (c + 1) * keep, :] = update[:, lanes]
            extra = jnp.where(row == c, total[2 * keep : 2 * keep + 1, lanes], extra)
        out_ref[part, share * keep :, :] = extra


def inverse_factor(square):
    size = square.shape[0]
    eye = (
        lax.broadcasted_iota(jnp.int32, (size, size), 0)
        == lax.broadcasted_iota(jnp.int32, (size, size), 1)
    ).astype(F32)
    both = jnp.concatenate([square, eye], 1)
    wide = (8, 2 * size)
    groups = size // 8
    rows = [both[8 * i : 8 * i + 8] for i in range(groups)]
    sublane = lax.broadcasted_iota(jnp.int32, wide, 0)
    done = []
    for j in range(groups):
        columns = [
            [jnp.broadcast_to(rows[i][:, 8 * j + k : 8 * j + k + 1], wide) for i in range(j, groups)]
            for k in range(8)
        ]
        scale = jnp.zeros(wide, F32)
        for k in range(8):
            pivot = jnp.broadcast_to(columns[k][0][k : k + 1], wide)
            scale = jnp.where(sublane == k, lax.rsqrt(pivot), scale)
            line = jnp.broadcast_to(rows[j][k : k + 1], wide) / pivot
            ratio = [
                jnp.broadcast_to(columns[k][0][m : m + 1], wide) / pivot for m in range(k + 1, 8)
            ]
            for i in range(j, groups):
                factor = columns[k][i - j]
                if i == j:
                    factor = jnp.where(sublane > k, factor, 0.0)
                rows[i] = rows[i] - factor * line
                for m in range(k + 1, 8):
                    columns[m][i - j] = columns[m][i - j] - factor * ratio[m - k - 1]
        done.append(rows[j] * scale)
    return jnp.concatenate(done, 0)[:, size:]


def basis_kernel(own_ref, other_ref, prior_ref, head_ref, tail_ref, far_ref,
                 basis_ref, pair_ref, shift_ref, head_out_ref, tail_out_ref, token_ref, sem):
    size = token_ref.shape[0] // sem.shape[0]

    def fetch(i):
        rows = pl.ds(pl.multiple_of(i * size, size), size)
        return pltpu.make_async_copy(far_ref.at[rows], token_ref.at[rows], sem.at[i])

    begin(fetch, sem.shape[0])
    core = lax.rem(lax.axis_index("region"), 2)
    keep = prior_ref.shape[0]
    share = prior_ref.shape[1] // 256
    own, other = own_ref[...], other_ref[...]
    halves = [jnp.where(core == part, own, other) for part in range(2)]
    update = jnp.concatenate([half[c * keep : (c + 1) * keep] for half in halves for c in range(share)], 1)
    base = share * keep
    sums = jnp.concatenate([half[base + c : base + c + 1] for half in halves for c in range(share)], 1)
    count = own[base + share : base + share + 1, :1]
    average = sums / count
    image = jnp.sum(prior_ref[...] * average, axis=1, keepdims=True)
    update = update - image * sums
    square = lax.dot_general(update, update, NT, precision=lax.Precision.HIGHEST, preferred_element_type=F32)
    inverse = inverse_factor(square)
    basis = lax.dot_general(inverse, update, NN, precision=lax.Precision.HIGHEST, preferred_element_type=F32)
    basis_ref[...] = basis
    high = basis.astype(BF16)
    low = (basis - high.astype(F32)).astype(BF16)
    pair = jnp.concatenate([high, low], 0).T
    pair_ref[...] = pair
    shift_ref[...] = jnp.broadcast_to(jnp.sum(basis * average, axis=1, keepdims=True), shift_ref.shape)
    for rows, out in ((head_ref, head_out_ref), (tail_ref, tail_out_ref)):
        wide = lax.dot_general(rows[...], pair, NN, preferred_element_type=F32).T
        out[...] = wide[:keep] + wide[keep:]
    for i in range(sem.shape[0]):
        fetch(i).wait()


def project_kernel(valid_ref, token_ref, pair_ref, shift_ref, out_ref, value_ref, out_sem, *, tok_rows):
    keep = shift_ref.shape[0]
    steps = tok_rows // STEP
    leave = []
    for step in range(steps):
        rows = pl.ds(step * STEP, STEP)
        wide = lax.dot_general(token_ref[rows, :], pair_ref[...], NN, preferred_element_type=F32).T
        place = step * STEP + lax.broadcasted_iota(jnp.int32, (1, STEP), 1)
        value = wide[:keep] + wide[keep:] - shift_ref[:, :1]
        value_ref[:, rows] = jnp.where(place < valid_ref[0], value, 0.0)
        leave.append(pltpu.make_async_copy(value_ref.at[:, rows], out_ref.at[:, rows], out_sem.at[step]))
        if step > 0:
            leave[step - 1].start()
    leave[steps - 1].start()
    for copy in leave:
        copy.wait()


def blend_kernel(width_ref, valid_ref, head_ref, tail_ref, before_ref, after_ref, shift_ref,
                 whole_ref, out_ref, buffer_ref, sem_ref, *, tok_rows, n_tile):
    left, right = widths(width_ref, n_tile)
    place = lax.broadcasted_iota(jnp.int32, (1, BAND), 1)
    shift = shift_ref[:, :1]
    before = pltpu.roll(before_ref[...], lax.rem(left, BAND), 1)
    after = pltpu.roll(after_ref[...], lax.rem(BAND - right, BAND), 1)
    head = jnp.where(place < left, (head_ref[...] + before) * 0.5, head_ref[...]) - shift
    tail = jnp.where(place >= BAND - right, (tail_ref[...] + after) * 0.5, tail_ref[...]) - shift
    start = tok_rows - BAND
    buffer_ref[0] = jnp.where(place < valid_ref[0], head, 0.0)
    buffer_ref[1] = jnp.where(start + place < valid_ref[0], tail, 0.0)
    first = pltpu.make_async_copy(buffer_ref.at[0], out_ref.at[:, pl.ds(0, BAND)], sem_ref.at[0])
    second = pltpu.make_async_copy(buffer_ref.at[1], out_ref.at[:, pl.ds(start, BAND)], sem_ref.at[1])
    first.start()
    second.start()
    first.wait()
    second.wait()


def smem():
    return pl.BlockSpec(memory_space=pltpu.SMEM)


def near():
    return pl.BlockSpec(memory_space=pltpu.VMEM)


def far():
    return pl.BlockSpec(memory_space=pltpu.HBM)


def params(mib):
    return pltpu.CompilerParams(vmem_limit_bytes=mib << 20)


def flip(value, mask):
    pairs = [(g, g ^ mask) for g in range(128)]
    return lax.ppermute(value, AXES, pairs)


def pick(stack, index):
    return lax.dynamic_index_in_dim(stack, index, 0, keepdims=False)


def reduce_all(halves):
    core = lax.axis_index("region") % 2
    mine = pick(halves, core) + flip(pick(halves, 1 - core), 32)
    for masks in ((2, 4, 6), (8, 16, 24), (1, 64, 65)):
        near_one, far_one, across = [flip(mine, mask) for mask in masks]
        mine = (mine + near_one) + (far_one + across)
    return mine, flip(mine, 32)


def per_device(quantized, block_scales, band_width, valid_count, prior_basis):
    tok_rows, feat_dim = quantized.shape
    keep = prior_basis.shape[1]
    groups = block_scales.shape[0]
    n_tile = lax.axis_size("tile")
    steps = tok_rows // STEP
    last = tok_rows // BAND - 1
    forward_pairs = [(i, i + 1) for i in range(n_tile - 1)]
    backward_pairs = [(i + 1, i) for i in range(n_tile - 1)]
    head_rows = pl.BlockSpec((BAND, feat_dim), lambda i: (0, 0))
    tail_rows = pl.BlockSpec((BAND, feat_dim), lambda i: (last, 0))

    def whole(*shape):
        return pl.BlockSpec(shape, lambda i: (0,) * len(shape))

    quant_far = pltpu.with_memory_space_constraint(quantized, pltpu.HBM)
    prior = prior_basis.T
    prior_far = pltpu.with_memory_space_constraint(prior, pltpu.HBM)
    scales_far = pltpu.with_memory_space_constraint(block_scales, pltpu.HBM)
    forward, backward, prior3, head_tokens, tail_tokens = pl.pallas_call(
        functools.partial(band_kernel, tok_rows=tok_rows),
        grid=(1,),
        in_specs=[
            smem(),
            head_rows,
            tail_rows,
            pl.BlockSpec((groups, BAND), lambda i: (0, 0)),
            pl.BlockSpec((groups, BAND), lambda i: (0, last)),
            whole(keep, feat_dim),
        ],
        out_specs=[
            whole(ROWS, BAND),
            whole(keep, BAND),
            whole(feat_dim, 4 * keep),
            whole(BAND, feat_dim),
            whole(BAND, feat_dim),
        ],
        out_shape=[
            jax.ShapeDtypeStruct((ROWS, BAND), F32),
            jax.ShapeDtypeStruct((keep, BAND), F32),
            jax.ShapeDtypeStruct((feat_dim, 4 * keep), BF16),
            jax.ShapeDtypeStruct((BAND, feat_dim), BF16),
            jax.ShapeDtypeStruct((BAND, feat_dim), BF16),
        ],
        compiler_params=params(24),
        name="band",
    )(valid_count, quant_far, quant_far, scales_far, scales_far, prior_far)
    before = lax.ppermute(forward, "tile", forward_pairs)
    after = lax.ppermute(backward, "tile", backward_pairs)
    bulk = pl.pallas_call(
        functools.partial(bulk_kernel, tok_rows=tok_rows, n_tile=n_tile),
        in_specs=[smem(), smem(), far(), near(), near()],
        out_specs=[far(), near()],
        out_shape=[
            pltpu.HBM((tok_rows, feat_dim), BF16),
            jax.ShapeDtypeStruct((2 * keep + 16, feat_dim), F32),
        ],
        scratch_shapes=[
            pltpu.VMEM((tok_rows, feat_dim), BF16),
            pltpu.VMEM((tok_rows, feat_dim), BF16),
            pltpu.SemaphoreType.DMA((steps,)),
            pltpu.SemaphoreType.DMA((steps,)),
        ],
        compiler_params=params(32),
        name="bulk",
    )
    tokens, sums = bulk(band_width, valid_count, quant_far, block_scales, prior3)
    pieces = pl.pallas_call(
        functools.partial(join_kernel, tok_rows=tok_rows, n_tile=n_tile),
        grid=(1,),
        in_specs=[
            smem(),
            smem(),
            whole(BAND, feat_dim),
            whole(BAND, feat_dim),
            whole(2 * keep + 16, feat_dim),
            whole(ROWS, BAND),
            whole(keep, BAND),
            whole(ROWS, BAND),
            whole(keep, BAND),
        ],
        out_specs=whole(2, feat_dim // 256 * keep + 8, 128),
        out_shape=jax.ShapeDtypeStruct((2, feat_dim // 256 * keep + 8, 128), F32),
        compiler_params=params(24),
        name="join",
    )(band_width, valid_count, head_tokens, tail_tokens, sums, forward, backward, before, after)
    own, other = reduce_all(pieces)
    basis, pair, shift, head, tail, tokens = pl.pallas_call(
        basis_kernel,
        in_specs=[near()] * 5 + [far()],
        out_specs=[near()] * 6,
        out_shape=[
            jax.ShapeDtypeStruct((keep, feat_dim), F32),
            jax.ShapeDtypeStruct((feat_dim, 2 * keep), BF16),
            jax.ShapeDtypeStruct((keep, 128), F32),
            jax.ShapeDtypeStruct((keep, BAND), F32),
            jax.ShapeDtypeStruct((keep, BAND), F32),
            jax.ShapeDtypeStruct((tok_rows, feat_dim), BF16),
        ],
        scratch_shapes=[pltpu.SemaphoreType.DMA((8,))],
        compiler_params=params(24),
        name="basis",
    )(own, other, prior, head_tokens, tail_tokens, pltpu.with_memory_space_constraint(tokens, pltpu.HBM))
    before = lax.ppermute(tail, "tile", forward_pairs)
    after = lax.ppermute(head, "tile", backward_pairs)
    raw = pl.pallas_call(
        functools.partial(project_kernel, tok_rows=tok_rows),
        in_specs=[smem(), near(), near(), near()],
        out_specs=far(),
        out_shape=pltpu.HBM((keep, tok_rows), F32),
        scratch_shapes=[pltpu.VMEM((keep, tok_rows), F32), pltpu.SemaphoreType.DMA((steps,))],
        compiler_params=params(20),
        name="project",
    )(valid_count, tokens, pair, shift)
    projected = pl.pallas_call(
        functools.partial(blend_kernel, tok_rows=tok_rows, n_tile=n_tile),
        in_specs=[smem(), smem()]
        + [pl.BlockSpec(memory_space=pltpu.VMEM)] * 5
        + [pl.BlockSpec(memory_space=pl.ANY)],
        out_specs=pl.BlockSpec(memory_space=pl.ANY),
        out_shape=jax.ShapeDtypeStruct((keep, tok_rows), F32),
        scratch_shapes=[pltpu.VMEM((2, keep, BAND), F32), pltpu.SemaphoreType.DMA((2,))],
        input_output_aliases={7: 0},
        compiler_params=params(8),
        name="blend",
    )(band_width, valid_count, head, tail, before, after, shift, raw)
    return projected, basis.T


def solution(mesh):
    return jax.shard_map(
        per_device,
        mesh=mesh,
        in_specs=(
            P(("region", "tile"), None),
            P(None, ("region", "tile")),
            P(),
            P(("region", "tile")),
            P(),
        ),
        out_specs=(P(None, ("region", "tile")), P()),
        check_vma=False,
    )
```

```python
import functools

import jax
import jax.numpy as jnp
from jax import lax
from jax.experimental import pallas as pl
from jax.experimental.pallas import tpu as pltpu
from jax.sharding import PartitionSpec as P


BAND = 256
STEP = 1024
ROWS = 72
AXES = ("region", "tile")
F32 = jnp.float32
BF16 = jnp.bfloat16
NT = (((1,), (1,)), ((), ()))
NN = (((1,), (0,)), ((), ()))


def split3(value):
    high = value.astype(BF16)
    rest = value - high.astype(F32)
    mid = rest.astype(BF16)
    low = (rest - mid.astype(F32)).astype(BF16)
    return high, mid, low


def dequantize(quant, scales):
    rows = quant.shape[0]
    groups = scales.shape[0]
    width = quant.shape[1] // groups
    return [
        (
            quant[:, b * width : (b + 1) * width].astype(F32)
            * jnp.broadcast_to(scales[b : b + 1], (width, rows)).T
        ).astype(BF16)
        for b in range(groups)
    ]


def reduced_rows(prior, tokens):
    wide = lax.dot_general(tokens, prior, NN, preferred_element_type=F32)
    half = (wide[:, :128] + wide[:, 128:]).T
    return half[:64] + half[64:]


def begin(count, *makers):
    def one(i, carry):
        for make in makers:
            make(i).start()
        return carry

    lax.fori_loop(0, count, one, 0)


def widths(width_ref, n_tile):
    tile = lax.axis_index("tile")
    number = lax.axis_index("region") * n_tile + tile
    left = jnp.where(tile > 0, width_ref[number], 0)
    last = width_ref.shape[0] - 1
    right = jnp.where(tile < n_tile - 1, width_ref[jnp.minimum(number + 1, last)], 0)
    return left, right


def band_kernel(valid_ref, head_ref, tail_ref, head_s_ref, tail_s_ref, prior_ref,
                forward_ref, backward_ref, prior3_ref, head_out_ref, tail_out_ref, *, tok_rows):
    high, mid, low = split3(prior_ref[...])
    prior = jnp.concatenate([high, mid, low, jnp.zeros_like(low)], 0).T
    prior3_ref[...] = prior
    head = jnp.concatenate(dequantize(head_ref[...], head_s_ref[...]), 1)
    head_out_ref[...] = head
    backward_ref[...] = reduced_rows(prior, head)
    tail = jnp.concatenate(dequantize(tail_ref[...], tail_s_ref[...]), 1)
    tail_out_ref[...] = tail
    keep = high.shape[0]
    forward_ref[:keep, :] = reduced_rows(prior, tail)
    place = tok_rows - BAND + lax.broadcasted_iota(jnp.int32, (ROWS - keep, BAND), 1)
    forward_ref[keep:, :] = jnp.where(place < valid_ref[0], 2.0, 1.0)


def bulk_kernel(width_ref, valid_ref, quant_ref, scale_ref, prior3_ref,
                token_ref, sum_ref, raw_ref, held_ref, in_sem, out_sem, *, tok_rows, n_tile):
    steps = tok_rows // STEP
    chunks = [pl.ds(step * STEP, STEP) for step in range(steps)]
    part = STEP // 2

    def mover(source, target, sems, step):
        def make(i):
            rows = pl.ds(pl.multiple_of(step * STEP + i * part, part), part)
            return pltpu.make_async_copy(source.at[rows], target.at[rows], sems.at[2 * step + i])

        return make

    arrive = [mover(quant_ref, raw_ref, in_sem, step) for step in range(steps)]
    leave = [mover(held_ref, token_ref, out_sem, step) for step in range(steps)]
    begin(2, arrive[0])
    begin(2, arrive[1])
    left, right = widths(width_ref, n_tile)
    for step in range(steps + 1):
        if step < steps:
            for i in range(2):
                arrive[step](i).wait()
        makers = [leave[step - 1]] if step > 0 else []
        if step + 2 < steps:
            makers.append(arrive[step + 2])
        if makers:
            begin(2, *makers)
        if step < steps:
            blocks = dequantize(raw_ref[chunks[step], :], scale_ref[:, chunks[step]])
            for b, block in enumerate(blocks):
                held_ref[chunks[step], b * block.shape[1] : (b + 1) * block.shape[1]] = block
        if step > 0:
            tokens = held_ref[chunks[step - 1], :]
            reduced = reduced_rows(prior3_ref[...], tokens)
            place = (step - 1) * STEP + lax.broadcasted_iota(jnp.int32, (1, STEP), 1)
            inner = (place >= left) & (place < tok_rows - right) & (place < valid_ref[0])
            weight = jnp.where(inner, 1.0, 0.0)
            reduced = reduced * weight
            high = reduced.astype(BF16)
            low = (reduced - high.astype(F32)).astype(BF16)
            extra = jnp.broadcast_to(weight, (16, STEP)).astype(BF16)
            total = lax.dot_general(
                jnp.concatenate([high, low, extra], 0), tokens, NN, preferred_element_type=F32
            )
            sum_ref[...] = total if step == 1 else sum_ref[...] + total
    for copies in leave:
        for i in range(2):
            copies(i).wait()


def join_kernel(width_ref, valid_ref, head_ref, tail_ref, sum_ref, forward_ref, backward_ref,
                before_ref, after_ref, out_ref, *, tok_rows, n_tile):
    left, right = widths(width_ref, n_tile)
    keep = backward_ref.shape[0]
    place = lax.broadcasted_iota(jnp.int32, (1, BAND), 1)
    before = pltpu.roll(before_ref[...], lax.rem(left, BAND), 1)
    after = pltpu.roll(after_ref[...], lax.rem(BAND - right, BAND), 1)
    count = jnp.where(place < left, before[keep : keep + 1], 0.0)
    head = (backward_ref[...] + before[:keep]) * (count * 0.25)
    both = jnp.where(place >= BAND - right, forward_ref[keep : keep + 1, :], 0.0)
    tail = (forward_ref[:keep, :] + after) * (both * 0.25)
    total = sum_ref[...]
    for reduced, weight, rows in ((head, count, head_ref), (tail, both, tail_ref)):
        reduced = jnp.where(weight > 0.0, reduced, 0.0)
        high = reduced.astype(BF16)
        low = (reduced - high.astype(F32)).astype(BF16)
        extra = jnp.broadcast_to(weight * 0.5, (16, BAND)).astype(BF16)
        total = total + lax.dot_general(
            jnp.concatenate([high, low, extra], 0), rows[...], NN, preferred_element_type=F32
        )
    update = total[:keep] + total[keep : 2 * keep]
    row = lax.broadcasted_iota(jnp.int32, (8, 128), 0)
    parts = out_ref.shape[0]
    share = total.shape[1] // 128 // parts
    for part in range(parts):
        extra = jnp.where(row == share, valid_ref[0].astype(F32), 0.0)
        for c in range(share):
            lanes = slice((part * share + c) * 128, (part * share + c + 1) * 128)
            out_ref[part, c * keep : (c + 1) * keep, :] = update[:, lanes]
            extra = jnp.where(row == c, total[2 * keep : 2 * keep + 1, lanes], extra)
        out_ref[part, share * keep :, :] = extra


def inverse_factor(square):
    size = square.shape[0]
    eye = (
        lax.broadcasted_iota(jnp.int32, (size, size), 0)
        == lax.broadcasted_iota(jnp.int32, (size, size), 1)
    ).astype(F32)
    both = jnp.concatenate([square, eye], 1)
    wide = (8, 2 * size)
    groups = size // 8
    rows = [both[8 * i : 8 * i + 8] for i in range(groups)]
    sublane = lax.broadcasted_iota(jnp.int32, wide, 0)
    done = []
    for j in range(groups):
        columns = [
            [jnp.broadcast_to(rows[i][:, 8 * j + k : 8 * j + k + 1], wide) for i in range(j, groups)]
            for k in range(8)
        ]
        scale = jnp.zeros(wide, F32)
        for k in range(8):
            pivot = jnp.broadcast_to(columns[k][0][k : k + 1], wide)
            scale = jnp.where(sublane == k, lax.rsqrt(pivot), scale)
            line = jnp.broadcast_to(rows[j][k : k + 1], wide) / pivot
            ratio = [
                jnp.broadcast_to(columns[k][0][m : m + 1], wide) / pivot for m in range(k + 1, 8)
            ]
            for i in range(j, groups):
                factor = columns[k][i - j]
                if i == j:
                    factor = jnp.where(sublane > k, factor, 0.0)
                rows[i] = rows[i] - factor * line
                for m in range(k + 1, 8):
                    columns[m][i - j] = columns[m][i - j] - factor * ratio[m - k - 1]
        done.append(rows[j] * scale)
    return jnp.concatenate(done, 0)[:, size:]


def basis_kernel(own_ref, other_ref, prior_ref, head_ref, tail_ref, far_ref,
                 basis_ref, pair_ref, shift_ref, head_out_ref, tail_out_ref, token_ref, sem):
    size = token_ref.shape[0] // sem.shape[0]

    def fetch(i):
        rows = pl.ds(pl.multiple_of(i * size, size), size)
        return pltpu.make_async_copy(far_ref.at[rows], token_ref.at[rows], sem.at[i])

    begin(sem.shape[0], fetch)
    core = lax.rem(lax.axis_index("region"), 2)
    keep = prior_ref.shape[0]
    share = prior_ref.shape[1] // 256
    own, other = own_ref[...], other_ref[...]
    halves = [jnp.where(core == part, own, other) for part in range(2)]
    update = jnp.concatenate([half[c * keep : (c + 1) * keep] for half in halves for c in range(share)], 1)
    base = share * keep
    sums = jnp.concatenate([half[base + c : base + c + 1] for half in halves for c in range(share)], 1)
    count = own[base + share : base + share + 1, :1]
    average = sums / count
    image = jnp.sum(prior_ref[...] * average, axis=1, keepdims=True)
    update = update - image * sums
    square = lax.dot_general(update, update, NT, precision=lax.Precision.HIGHEST, preferred_element_type=F32)
    inverse = inverse_factor(square)
    basis = lax.dot_general(inverse, update, NN, precision=lax.Precision.HIGHEST, preferred_element_type=F32)
    basis_ref[...] = basis
    high = basis.astype(BF16)
    low = (basis - high.astype(F32)).astype(BF16)
    pair = jnp.concatenate([high, low], 0).T
    pair_ref[...] = pair
    shift_ref[...] = jnp.broadcast_to(jnp.sum(basis * average, axis=1, keepdims=True), shift_ref.shape)
    for rows, out in ((head_ref, head_out_ref), (tail_ref, tail_out_ref)):
        wide = lax.dot_general(rows[...], pair, NN, preferred_element_type=F32).T
        out[...] = wide[:keep] + wide[keep:]
    for i in range(sem.shape[0]):
        fetch(i).wait()


def project_kernel(valid_ref, early_ref, far_ref, pair_ref, shift_ref, basis_ref,
                   out_ref, basis_out_ref, late_ref, value_ref, in_sem, out_sem, *, tok_rows):
    keep = shift_ref.shape[0]
    steps = tok_rows // STEP
    half = early_ref.shape[0]

    def fetch(i):
        rows = pl.multiple_of(i * STEP, STEP)
        return pltpu.make_async_copy(far_ref.at[pl.ds(half + rows, STEP)], late_ref.at[pl.ds(rows, STEP)], in_sem.at[i])

    begin((tok_rows - half) // STEP, fetch)
    leave = [pltpu.make_async_copy(basis_ref, basis_out_ref, out_sem.at[steps])]
    leave[0].start()
    for step in range(steps):
        lanes = pl.ds(step * STEP, STEP)
        if step * STEP < half:
            tokens = early_ref[lanes, :]
        else:
            fetch(step - half // STEP).wait()
            tokens = late_ref[pl.ds(step * STEP - half, STEP), :]
        wide = lax.dot_general(tokens, pair_ref[...], NN, preferred_element_type=F32).T
        place = step * STEP + lax.broadcasted_iota(jnp.int32, (1, STEP), 1)
        value = wide[:keep] + wide[keep:] - shift_ref[:, :1]
        value_ref[:, lanes] = jnp.where(place < valid_ref[0], value, 0.0)
        leave.append(pltpu.make_async_copy(value_ref.at[:, lanes], out_ref.at[:, lanes], out_sem.at[step]))
        if step > 0:
            leave[step].start()
    leave[steps].start()
    for copy in leave:
        copy.wait()


def blend_kernel(width_ref, valid_ref, head_ref, tail_ref, before_ref, after_ref, shift_ref,
                 whole_ref, out_ref, buffer_ref, sem_ref, *, tok_rows, n_tile):
    left, right = widths(width_ref, n_tile)
    place = lax.broadcasted_iota(jnp.int32, (1, BAND), 1)
    shift = shift_ref[:, :1]
    before = pltpu.roll(before_ref[...], lax.rem(left, BAND), 1)
    after = pltpu.roll(after_ref[...], lax.rem(BAND - right, BAND), 1)
    head = jnp.where(place < left, (head_ref[...] + before) * 0.5, head_ref[...]) - shift
    tail = jnp.where(place >= BAND - right, (tail_ref[...] + after) * 0.5, tail_ref[...]) - shift
    start = tok_rows - BAND
    buffer_ref[0] = jnp.where(place < valid_ref[0], head, 0.0)
    buffer_ref[1] = jnp.where(start + place < valid_ref[0], tail, 0.0)
    first = pltpu.make_async_copy(buffer_ref.at[0], out_ref.at[:, pl.ds(0, BAND)], sem_ref.at[0])
    second = pltpu.make_async_copy(buffer_ref.at[1], out_ref.at[:, pl.ds(start, BAND)], sem_ref.at[1])
    first.start()
    second.start()
    first.wait()
    second.wait()


def smem():
    return pl.BlockSpec(memory_space=pltpu.SMEM)


def near():
    return pl.BlockSpec(memory_space=pltpu.VMEM)


def far():
    return pl.BlockSpec(memory_space=pltpu.HBM)


def params(mib):
    return pltpu.CompilerParams(vmem_limit_bytes=mib << 20)


def flip(value, mask):
    pairs = [(g, g ^ mask) for g in range(128)]
    return lax.ppermute(value, AXES, pairs)


def pick(stack, index):
    return lax.dynamic_index_in_dim(stack, index, 0, keepdims=False)


def reduce_all(halves):
    core = lax.axis_index("region") % 2
    mine = pick(halves, core) + flip(pick(halves, 1 - core), 32)
    for masks in ((2, 4, 6), (8, 16, 24), (1, 64, 65)):
        near_one, far_one, across = [flip(mine, mask) for mask in masks]
        mine = (mine + near_one) + (far_one + across)
    return mine, flip(mine, 32)


def per_device(quantized, block_scales, band_width, valid_count, prior_basis):
    tok_rows, feat_dim = quantized.shape
    keep = prior_basis.shape[1]
    groups = block_scales.shape[0]
    n_tile = lax.axis_size("tile")
    steps = tok_rows // STEP
    last = tok_rows // BAND - 1
    forward_pairs = [(i, i + 1) for i in range(n_tile - 1)]
    backward_pairs = [(i + 1, i) for i in range(n_tile - 1)]
    head_rows = pl.BlockSpec((BAND, feat_dim), lambda i: (0, 0))
    tail_rows = pl.BlockSpec((BAND, feat_dim), lambda i: (last, 0))

    def whole(*shape):
        return pl.BlockSpec(shape, lambda i: (0,) * len(shape))

    quant_far = pltpu.with_memory_space_constraint(quantized, pltpu.HBM)
    prior = prior_basis.T
    prior_far = pltpu.with_memory_space_constraint(prior, pltpu.HBM)
    scales_far = pltpu.with_memory_space_constraint(block_scales, pltpu.HBM)
    forward, backward, prior3, head_tokens, tail_tokens = pl.pallas_call(
        functools.partial(band_kernel, tok_rows=tok_rows),
        grid=(1,),
        in_specs=[
            smem(),
            head_rows,
            tail_rows,
            pl.BlockSpec((groups, BAND), lambda i: (0, 0)),
            pl.BlockSpec((groups, BAND), lambda i: (0, last)),
            whole(keep, feat_dim),
        ],
        out_specs=[
            whole(ROWS, BAND),
            whole(keep, BAND),
            whole(feat_dim, 4 * keep),
            whole(BAND, feat_dim),
            whole(BAND, feat_dim),
        ],
        out_shape=[
            jax.ShapeDtypeStruct((ROWS, BAND), F32),
            jax.ShapeDtypeStruct((keep, BAND), F32),
            jax.ShapeDtypeStruct((feat_dim, 4 * keep), BF16),
            jax.ShapeDtypeStruct((BAND, feat_dim), BF16),
            jax.ShapeDtypeStruct((BAND, feat_dim), BF16),
        ],
        compiler_params=params(24),
        name="band",
    )(valid_count, quant_far, quant_far, scales_far, scales_far, prior_far)
    before = lax.ppermute(forward, "tile", forward_pairs)
    after = lax.ppermute(backward, "tile", backward_pairs)
    bulk = pl.pallas_call(
        functools.partial(bulk_kernel, tok_rows=tok_rows, n_tile=n_tile),
        in_specs=[smem(), smem(), far(), near(), near()],
        out_specs=[far(), near()],
        out_shape=[
            pltpu.HBM((tok_rows, feat_dim), BF16),
            jax.ShapeDtypeStruct((2 * keep + 16, feat_dim), F32),
        ],
        scratch_shapes=[
            pltpu.VMEM((tok_rows, feat_dim), BF16),
            pltpu.VMEM((tok_rows, feat_dim), BF16),
            pltpu.SemaphoreType.DMA((2 * steps,)),
            pltpu.SemaphoreType.DMA((2 * steps,)),
        ],
        compiler_params=params(32),
        name="bulk",
    )
    tokens, sums = bulk(band_width, valid_count, quant_far, block_scales, prior3)
    pieces = pl.pallas_call(
        functools.partial(join_kernel, tok_rows=tok_rows, n_tile=n_tile),
        grid=(1,),
        in_specs=[
            smem(),
            smem(),
            whole(BAND, feat_dim),
            whole(BAND, feat_dim),
            whole(2 * keep + 16, feat_dim),
            whole(ROWS, BAND),
            whole(keep, BAND),
            whole(ROWS, BAND),
            whole(keep, BAND),
        ],
        out_specs=whole(2, feat_dim // 256 * keep + 8, 128),
        out_shape=jax.ShapeDtypeStruct((2, feat_dim // 256 * keep + 8, 128), F32),
        compiler_params=params(24),
        name="join",
    )(band_width, valid_count, head_tokens, tail_tokens, sums, forward, backward, before, after)
    own, other = reduce_all(pieces)
    tokens = pltpu.with_memory_space_constraint(tokens, pltpu.HBM)
    basis, pair, shift, head, tail, early = pl.pallas_call(
        basis_kernel,
        in_specs=[near()] * 5 + [far()],
        out_specs=[near()] * 6,
        out_shape=[
            jax.ShapeDtypeStruct((keep, feat_dim), F32),
            jax.ShapeDtypeStruct((feat_dim, 2 * keep), BF16),
            jax.ShapeDtypeStruct((keep, 128), F32),
            jax.ShapeDtypeStruct((keep, BAND), F32),
            jax.ShapeDtypeStruct((keep, BAND), F32),
            jax.ShapeDtypeStruct((tok_rows // 2, feat_dim), BF16),
        ],
        scratch_shapes=[pltpu.SemaphoreType.DMA((4,))],
        compiler_params=params(24),
        name="basis",
    )(own, other, prior, head_tokens, tail_tokens, tokens)
    before = lax.ppermute(tail, "tile", forward_pairs)
    after = lax.ppermute(head, "tile", backward_pairs)
    raw, basis = pl.pallas_call(
        functools.partial(project_kernel, tok_rows=tok_rows),
        in_specs=[smem(), near(), far(), near(), near(), near()],
        out_specs=[far(), far()],
        out_shape=[pltpu.HBM((keep, tok_rows), F32), pltpu.HBM((keep, feat_dim), F32)],
        scratch_shapes=[
            pltpu.VMEM((tok_rows // 2, feat_dim), BF16),
            pltpu.VMEM((keep, tok_rows), F32),
            pltpu.SemaphoreType.DMA((steps // 2,)),
            pltpu.SemaphoreType.DMA((steps + 1,)),
        ],
        compiler_params=params(24),
        name="project",
    )(valid_count, early, tokens, pair, shift, basis)
    projected = pl.pallas_call(
        functools.partial(blend_kernel, tok_rows=tok_rows, n_tile=n_tile),
        in_specs=[smem(), smem()]
        + [pl.BlockSpec(memory_space=pltpu.VMEM)] * 5
        + [pl.BlockSpec(memory_space=pl.ANY)],
        out_specs=pl.BlockSpec(memory_space=pl.ANY),
        out_shape=jax.ShapeDtypeStruct((keep, tok_rows), F32),
        scratch_shapes=[pltpu.VMEM((2, keep, BAND), F32), pltpu.SemaphoreType.DMA((2,))],
        input_output_aliases={7: 0},
        compiler_params=params(8),
        name="blend",
    )(band_width, valid_count, head, tail, before, after, shift, raw)
    return projected, basis.T


def solution(mesh):
    return jax.shard_map(
        per_device,
        mesh=mesh,
        in_specs=(
            P(("region", "tile"), None),
            P(None, ("region", "tile")),
            P(),
            P(("region", "tile")),
            P(),
        ),
        out_specs=(P(None, ("region", "tile")), P()),
        check_vma=False,
    )
```

```python
import functools

import jax
import jax.numpy as jnp
from jax import lax
from jax.experimental import pallas as pl
from jax.experimental.pallas import tpu as pltpu
from jax.sharding import PartitionSpec as P


BAND = 256
STEP = 1024
ROWS = 72
AXES = ("region", "tile")
F32 = jnp.float32
BF16 = jnp.bfloat16
NT = (((1,), (1,)), ((), ()))
NN = (((1,), (0,)), ((), ()))


def split3(value):
    high = value.astype(BF16)
    rest = value - high.astype(F32)
    mid = rest.astype(BF16)
    low = (rest - mid.astype(F32)).astype(BF16)
    return high, mid, low


def dequantize(quant, scales):
    rows = quant.shape[0]
    groups = scales.shape[0]
    width = quant.shape[1] // groups
    return [
        (
            quant[:, b * width : (b + 1) * width].astype(F32)
            * jnp.broadcast_to(scales[b : b + 1], (width, rows)).T
        ).astype(BF16)
        for b in range(groups)
    ]


def reduced_rows(prior, tokens):
    wide = lax.dot_general(tokens, prior, NN, preferred_element_type=F32)
    half = (wide[:, :128] + wide[:, 128:]).T
    return half[:64] + half[64:]


def begin(count, *makers):
    def one(i, carry):
        for make in makers:
            make(i).start()
        return carry

    lax.fori_loop(0, count, one, 0)


def widths(width_ref, n_tile):
    tile = lax.axis_index("tile")
    number = lax.axis_index("region") * n_tile + tile
    left = jnp.where(tile > 0, width_ref[number], 0)
    last = width_ref.shape[0] - 1
    right = jnp.where(tile < n_tile - 1, width_ref[jnp.minimum(number + 1, last)], 0)
    return left, right


def band_kernel(valid_ref, head_ref, tail_ref, head_s_ref, tail_s_ref, prior_ref,
                forward_ref, backward_ref, prior3_ref, head_out_ref, tail_out_ref, *, tok_rows):
    high, mid, low = split3(prior_ref[...])
    prior = jnp.concatenate([high, mid, low, jnp.zeros_like(low)], 0).T
    prior3_ref[...] = prior
    head = jnp.concatenate(dequantize(head_ref[...], head_s_ref[...]), 1)
    head_out_ref[...] = head
    backward_ref[...] = reduced_rows(prior, head)
    tail = jnp.concatenate(dequantize(tail_ref[...], tail_s_ref[...]), 1)
    tail_out_ref[...] = tail
    keep = high.shape[0]
    forward_ref[:keep, :] = reduced_rows(prior, tail)
    place = tok_rows - BAND + lax.broadcasted_iota(jnp.int32, (ROWS - keep, BAND), 1)
    forward_ref[keep:, :] = jnp.where(place < valid_ref[0], 2.0, 1.0)


def bulk_kernel(width_ref, valid_ref, quant_ref, scale_ref, prior3_ref,
                token_ref, sum_ref, raw_ref, held_ref, in_sem, out_sem, *, tok_rows, n_tile):
    steps = tok_rows // STEP
    chunks = [pl.ds(step * STEP, STEP) for step in range(steps)]
    part = STEP // 2

    def mover(source, target, sems, step):
        def make(i):
            rows = pl.ds(pl.multiple_of(step * STEP + i * part, part), part)
            return pltpu.make_async_copy(source.at[rows], target.at[rows], sems.at[2 * step + i])

        return make

    arrive = [mover(quant_ref, raw_ref, in_sem, step) for step in range(steps)]
    leave = [mover(held_ref, token_ref, out_sem, step) for step in range(steps)]
    begin(2, arrive[0])
    begin(2, arrive[1])
    left, right = widths(width_ref, n_tile)
    for step in range(steps + 1):
        if step < steps:
            for i in range(2):
                arrive[step](i).wait()
        makers = [leave[step - 1]] if step > 0 else []
        if step + 2 < steps:
            makers.append(arrive[step + 2])
        if makers:
            begin(2, *makers)
        if step < steps:
            blocks = dequantize(raw_ref[chunks[step], :], scale_ref[:, chunks[step]])
            for b, block in enumerate(blocks):
                held_ref[chunks[step], b * block.shape[1] : (b + 1) * block.shape[1]] = block
        if step > 0:
            tokens = held_ref[chunks[step - 1], :]
            reduced = reduced_rows(prior3_ref[...], tokens)
            place = (step - 1) * STEP + lax.broadcasted_iota(jnp.int32, (1, STEP), 1)
            inner = (place >= left) & (place < tok_rows - right) & (place < valid_ref[0])
            weight = jnp.where(inner, 1.0, 0.0)
            reduced = reduced * weight
            high = reduced.astype(BF16)
            low = (reduced - high.astype(F32)).astype(BF16)
            extra = jnp.broadcast_to(weight, (16, STEP)).astype(BF16)
            total = lax.dot_general(
                jnp.concatenate([high, low, extra], 0), tokens, NN, preferred_element_type=F32
            )
            sum_ref[...] = total if step == 1 else sum_ref[...] + total
    for copies in leave:
        for i in range(2):
            copies(i).wait()


def join_kernel(width_ref, valid_ref, head_ref, tail_ref, sum_ref, forward_ref, backward_ref,
                before_ref, after_ref, out_ref, *, tok_rows, n_tile):
    left, right = widths(width_ref, n_tile)
    keep = backward_ref.shape[0]
    place = lax.broadcasted_iota(jnp.int32, (1, BAND), 1)
    before = pltpu.roll(before_ref[...], lax.rem(left, BAND), 1)
    after = pltpu.roll(after_ref[...], lax.rem(BAND - right, BAND), 1)
    count = jnp.where(place < left, before[keep : keep + 1], 0.0)
    head = (backward_ref[...] + before[:keep]) * (count * 0.25)
    both = jnp.where(place >= BAND - right, forward_ref[keep : keep + 1, :], 0.0)
    tail = (forward_ref[:keep, :] + after) * (both * 0.25)
    total = sum_ref[...]
    for reduced, weight, rows in ((head, count, head_ref), (tail, both, tail_ref)):
        reduced = jnp.where(weight > 0.0, reduced, 0.0)
        high = reduced.astype(BF16)
        low = (reduced - high.astype(F32)).astype(BF16)
        extra = jnp.broadcast_to(weight * 0.5, (16, BAND)).astype(BF16)
        total = total + lax.dot_general(
            jnp.concatenate([high, low, extra], 0), rows[...], NN, preferred_element_type=F32
        )
    update = total[:keep] + total[keep : 2 * keep]
    row = lax.broadcasted_iota(jnp.int32, (8, 128), 0)
    parts = out_ref.shape[0]
    share = total.shape[1] // 128 // parts
    for part in range(parts):
        extra = jnp.where(row == share, valid_ref[0].astype(F32), 0.0)
        for c in range(share):
            lanes = slice((part * share + c) * 128, (part * share + c + 1) * 128)
            out_ref[part, c * keep : (c + 1) * keep, :] = update[:, lanes]
            extra = jnp.where(row == c, total[2 * keep : 2 * keep + 1, lanes], extra)
        out_ref[part, share * keep :, :] = extra


def inverse_factor(square):
    size = square.shape[0]
    eye = (
        lax.broadcasted_iota(jnp.int32, (size, size), 0)
        == lax.broadcasted_iota(jnp.int32, (size, size), 1)
    ).astype(F32)
    both = jnp.concatenate([square, eye], 1)
    wide = (8, 2 * size)
    groups = size // 8
    rows = [both[8 * i : 8 * i + 8] for i in range(groups)]
    sublane = lax.broadcasted_iota(jnp.int32, wide, 0)
    done = []
    for j in range(groups):
        columns = [
            [jnp.broadcast_to(rows[i][:, 8 * j + k : 8 * j + k + 1], wide) for i in range(j, groups)]
            for k in range(8)
        ]
        scale = jnp.zeros(wide, F32)
        for k in range(8):
            pivot = jnp.broadcast_to(columns[k][0][k : k + 1], wide)
            scale = jnp.where(sublane == k, lax.rsqrt(pivot), scale)
            line = jnp.broadcast_to(rows[j][k : k + 1], wide) / pivot
            ratio = [
                jnp.broadcast_to(columns[k][0][m : m + 1], wide) / pivot for m in range(k + 1, 8)
            ]
            for i in range(j, groups):
                factor = columns[k][i - j]
                if i == j:
                    factor = jnp.where(sublane > k, factor, 0.0)
                rows[i] = rows[i] - factor * line
                for m in range(k + 1, 8):
                    columns[m][i - j] = columns[m][i - j] - factor * ratio[m - k - 1]
        done.append(rows[j] * scale)
    return jnp.concatenate(done, 0)[:, size:]


def basis_kernel(own_ref, other_ref, prior_ref, head_ref, tail_ref, far_ref,
                 basis_ref, pair_ref, shift_ref, head_out_ref, tail_out_ref, token_ref, sem):
    size = token_ref.shape[0] // sem.shape[0]

    def fetch(i):
        rows = pl.ds(pl.multiple_of(i * size, size), size)
        return pltpu.make_async_copy(far_ref.at[rows], token_ref.at[rows], sem.at[i])

    begin(sem.shape[0], fetch)
    core = lax.rem(lax.axis_index("region"), 2)
    keep = prior_ref.shape[0]
    share = prior_ref.shape[1] // 256
    own, other = own_ref[...], other_ref[...]
    halves = [jnp.where(core == part, own, other) for part in range(2)]
    update = jnp.concatenate([half[c * keep : (c + 1) * keep] for half in halves for c in range(share)], 1)
    base = share * keep
    sums = jnp.concatenate([half[base + c : base + c + 1] for half in halves for c in range(share)], 1)
    count = own[base + share : base + share + 1, :1]
    average = sums / count
    image = jnp.sum(prior_ref[...] * average, axis=1, keepdims=True)
    update = update - image * sums
    square = lax.dot_general(update, update, NT, precision=lax.Precision.HIGHEST, preferred_element_type=F32)
    inverse = inverse_factor(square)
    basis = lax.dot_general(inverse, update, NN, precision=lax.Precision.HIGHEST, preferred_element_type=F32)
    basis_ref[...] = basis
    high = basis.astype(BF16)
    low = (basis - high.astype(F32)).astype(BF16)
    pair = jnp.concatenate([high, low], 0).T
    pair_ref[...] = pair
    shift_ref[...] = jnp.broadcast_to(jnp.sum(basis * average, axis=1, keepdims=True), shift_ref.shape)
    for rows, out in ((head_ref, head_out_ref), (tail_ref, tail_out_ref)):
        wide = lax.dot_general(rows[...], pair, NN, preferred_element_type=F32).T
        out[...] = wide[:keep] + wide[keep:]
    for i in range(sem.shape[0]):
        fetch(i).wait()


def project_kernel(valid_ref, early_ref, far_ref, pair_ref, shift_ref, basis_ref,
                   out_ref, basis_out_ref, late_ref, value_ref, in_sem, out_sem, *, tok_rows):
    keep = shift_ref.shape[0]
    steps = tok_rows // STEP
    half = early_ref.shape[0]

    size = (tok_rows - half) // 4

    def fetch(i):
        rows = pl.multiple_of(i * size, size)
        return pltpu.make_async_copy(far_ref.at[pl.ds(half + rows, size)], late_ref.at[pl.ds(rows, size)], in_sem.at[i])

    begin(4, fetch)
    leave = [pltpu.make_async_copy(basis_ref, basis_out_ref, out_sem.at[steps])]
    leave[0].start()
    for step in range(steps):
        lanes = pl.ds(step * STEP, STEP)
        if step * STEP < half:
            tokens = early_ref[lanes, :]
        else:
            for i in range(4):
                fetch(i).wait()
            tokens = late_ref[...]
        wide = lax.dot_general(tokens, pair_ref[...], NN, preferred_element_type=F32).T
        place = step * STEP + lax.broadcasted_iota(jnp.int32, (1, STEP), 1)
        value = wide[:keep] + wide[keep:] - shift_ref[:, :1]
        value_ref[:, lanes] = jnp.where(place < valid_ref[0], value, 0.0)
        leave.append(pltpu.make_async_copy(value_ref.at[:, lanes], out_ref.at[:, lanes], out_sem.at[step]))
        if step > 0:
            leave[step].start()
    leave[steps].start()
    for copy in leave:
        copy.wait()


def blend_kernel(width_ref, valid_ref, head_ref, tail_ref, before_ref, after_ref, shift_ref,
                 whole_ref, out_ref, buffer_ref, sem_ref, *, tok_rows, n_tile):
    left, right = widths(width_ref, n_tile)
    place = lax.broadcasted_iota(jnp.int32, (1, BAND), 1)
    shift = shift_ref[:, :1]
    before = pltpu.roll(before_ref[...], lax.rem(left, BAND), 1)
    after = pltpu.roll(after_ref[...], lax.rem(BAND - right, BAND), 1)
    head = jnp.where(place < left, (head_ref[...] + before) * 0.5, head_ref[...]) - shift
    tail = jnp.where(place >= BAND - right, (tail_ref[...] + after) * 0.5, tail_ref[...]) - shift
    start = tok_rows - BAND
    buffer_ref[0] = jnp.where(place < valid_ref[0], head, 0.0)
    buffer_ref[1] = jnp.where(start + place < valid_ref[0], tail, 0.0)
    first = pltpu.make_async_copy(buffer_ref.at[0], out_ref.at[:, pl.ds(0, BAND)], sem_ref.at[0])
    second = pltpu.make_async_copy(buffer_ref.at[1], out_ref.at[:, pl.ds(start, BAND)], sem_ref.at[1])
    first.start()
    second.start()
    first.wait()
    second.wait()


def smem():
    return pl.BlockSpec(memory_space=pltpu.SMEM)


def near():
    return pl.BlockSpec(memory_space=pltpu.VMEM)


def far():
    return pl.BlockSpec(memory_space=pltpu.HBM)


def params(mib):
    return pltpu.CompilerParams(vmem_limit_bytes=mib << 20)


def flip(value, masks):
    pairs = [(g, g ^ masks[(g >> 5) & 1]) for g in range(128)]
    return lax.ppermute(value, AXES, pairs)


def pick(stack, index):
    return lax.dynamic_index_in_dim(stack, index, 0, keepdims=False)


def reduce_all(halves):
    core = lax.axis_index("region") % 2
    both = (32, 32)
    mine = pick(halves, core) + flip(pick(halves, 1 - core), both)
    along_y, along_x, along_z = (2, 4, 6), (8, 16, 24), (1, 64, 65)
    for stage in ((along_y, along_x), (along_x, along_z), (along_z, along_y)):
        near_one, far_one, across = [flip(mine, masks) for masks in zip(*stage)]
        mine = (mine + near_one) + (far_one + across)
    return mine, flip(mine, both)


def per_device(quantized, block_scales, band_width, valid_count, prior_basis):
    tok_rows, feat_dim = quantized.shape
    keep = prior_basis.shape[1]
    groups = block_scales.shape[0]
    n_tile = lax.axis_size("tile")
    steps = tok_rows // STEP
    last = tok_rows // BAND - 1
    forward_pairs = [(i, i + 1) for i in range(n_tile - 1)]
    backward_pairs = [(i + 1, i) for i in range(n_tile - 1)]
    head_rows = pl.BlockSpec((BAND, feat_dim), lambda i: (0, 0))
    tail_rows = pl.BlockSpec((BAND, feat_dim), lambda i: (last, 0))

    def whole(*shape):
        return pl.BlockSpec(shape, lambda i: (0,) * len(shape))

    quant_far = pltpu.with_memory_space_constraint(quantized, pltpu.HBM)
    prior = prior_basis.T
    prior_far = pltpu.with_memory_space_constraint(prior, pltpu.HBM)
    scales_far = pltpu.with_memory_space_constraint(block_scales, pltpu.HBM)
    forward, backward, prior3, head_tokens, tail_tokens = pl.pallas_call(
        functools.partial(band_kernel, tok_rows=tok_rows),
        grid=(1,),
        in_specs=[
            smem(),
            head_rows,
            tail_rows,
            pl.BlockSpec((groups, BAND), lambda i: (0, 0)),
            pl.BlockSpec((groups, BAND), lambda i: (0, last)),
            whole(keep, feat_dim),
        ],
        out_specs=[
            whole(ROWS, BAND),
            whole(keep, BAND),
            whole(feat_dim, 4 * keep),
            whole(BAND, feat_dim),
            whole(BAND, feat_dim),
        ],
        out_shape=[
            jax.ShapeDtypeStruct((ROWS, BAND), F32),
            jax.ShapeDtypeStruct((keep, BAND), F32),
            jax.ShapeDtypeStruct((feat_dim, 4 * keep), BF16),
            jax.ShapeDtypeStruct((BAND, feat_dim), BF16),
            jax.ShapeDtypeStruct((BAND, feat_dim), BF16),
        ],
        compiler_params=params(24),
        name="band",
    )(valid_count, quant_far, quant_far, scales_far, scales_far, prior_far)
    before = lax.ppermute(forward, "tile", forward_pairs)
    after = lax.ppermute(backward, "tile", backward_pairs)
    bulk = pl.pallas_call(
        functools.partial(bulk_kernel, tok_rows=tok_rows, n_tile=n_tile),
        in_specs=[smem(), smem(), far(), near(), near()],
        out_specs=[far(), near()],
        out_shape=[
            pltpu.HBM((tok_rows, feat_dim), BF16),
            jax.ShapeDtypeStruct((2 * keep + 16, feat_dim), F32),
        ],
        scratch_shapes=[
            pltpu.VMEM((tok_rows, feat_dim), BF16),
            pltpu.VMEM((tok_rows, feat_dim), BF16),
            pltpu.SemaphoreType.DMA((2 * steps,)),
            pltpu.SemaphoreType.DMA((2 * steps,)),
        ],
        compiler_params=params(32),
        name="bulk",
    )
    tokens, sums = bulk(band_width, valid_count, quant_far, block_scales, prior3)
    pieces = pl.pallas_call(
        functools.partial(join_kernel, tok_rows=tok_rows, n_tile=n_tile),
        grid=(1,),
        in_specs=[
            smem(),
            smem(),
            whole(BAND, feat_dim),
            whole(BAND, feat_dim),
            whole(2 * keep + 16, feat_dim),
            whole(ROWS, BAND),
            whole(keep, BAND),
            whole(ROWS, BAND),
            whole(keep, BAND),
        ],
        out_specs=whole(2, feat_dim // 256 * keep + 8, 128),
        out_shape=jax.ShapeDtypeStruct((2, feat_dim // 256 * keep + 8, 128), F32),
        compiler_params=params(24),
        name="join",
    )(band_width, valid_count, head_tokens, tail_tokens, sums, forward, backward, before, after)
    own, other = reduce_all(pieces)
    tokens = pltpu.with_memory_space_constraint(tokens, pltpu.HBM)
    basis, pair, shift, head, tail, early = pl.pallas_call(
        basis_kernel,
        in_specs=[near()] * 5 + [far()],
        out_specs=[near()] * 6,
        out_shape=[
            jax.ShapeDtypeStruct((keep, feat_dim), F32),
            jax.ShapeDtypeStruct((feat_dim, 2 * keep), BF16),
            jax.ShapeDtypeStruct((keep, 128), F32),
            jax.ShapeDtypeStruct((keep, BAND), F32),
            jax.ShapeDtypeStruct((keep, BAND), F32),
            jax.ShapeDtypeStruct((tok_rows - STEP, feat_dim), BF16),
        ],
        scratch_shapes=[pltpu.SemaphoreType.DMA((6,))],
        compiler_params=params(24),
        name="basis",
    )(own, other, prior, head_tokens, tail_tokens, tokens)
    before = lax.ppermute(tail, "tile", forward_pairs)
    after = lax.ppermute(head, "tile", backward_pairs)
    raw, basis = pl.pallas_call(
        functools.partial(project_kernel, tok_rows=tok_rows),
        in_specs=[smem(), near(), far(), near(), near(), near()],
        out_specs=[far(), far()],
        out_shape=[pltpu.HBM((keep, tok_rows), F32), pltpu.HBM((keep, feat_dim), F32)],
        scratch_shapes=[
            pltpu.VMEM((STEP, feat_dim), BF16),
            pltpu.VMEM((keep, tok_rows), F32),
            pltpu.SemaphoreType.DMA((4,)),
            pltpu.SemaphoreType.DMA((steps + 1,)),
        ],
        compiler_params=params(24),
        name="project",
    )(valid_count, early, tokens, pair, shift, basis)
    projected = pl.pallas_call(
        functools.partial(blend_kernel, tok_rows=tok_rows, n_tile=n_tile),
        in_specs=[smem(), smem()]
        + [pl.BlockSpec(memory_space=pltpu.VMEM)] * 5
        + [pl.BlockSpec(memory_space=pl.ANY)],
        out_specs=pl.BlockSpec(memory_space=pl.ANY),
        out_shape=jax.ShapeDtypeStruct((keep, tok_rows), F32),
        scratch_shapes=[pltpu.VMEM((2, keep, BAND), F32), pltpu.SemaphoreType.DMA((2,))],
        input_output_aliases={7: 0},
        compiler_params=params(8),
        name="blend",
    )(band_width, valid_count, head, tail, before, after, shift, raw)
    return projected, basis.T


def solution(mesh):
    return jax.shard_map(
        per_device,
        mesh=mesh,
        in_specs=(
            P(("region", "tile"), None),
            P(None, ("region", "tile")),
            P(),
            P(("region", "tile")),
            P(),
        ),
        out_specs=(P(None, ("region", "tile")), P()),
        check_vma=False,
    )
```

```python
import functools

import jax
import jax.numpy as jnp
from jax import lax
from jax.experimental import pallas as pl
from jax.experimental.pallas import tpu as pltpu
from jax.sharding import PartitionSpec as P


BAND = 256
STEP = 1024
ROWS = 72
AXES = ("region", "tile")
F32 = jnp.float32
BF16 = jnp.bfloat16
NT = (((1,), (1,)), ((), ()))
NN = (((1,), (0,)), ((), ()))


def split3(value):
    high = value.astype(BF16)
    rest = value - high.astype(F32)
    mid = rest.astype(BF16)
    low = (rest - mid.astype(F32)).astype(BF16)
    return high, mid, low


def dequantize(quant, scales):
    rows = quant.shape[0]
    groups = scales.shape[0]
    width = quant.shape[1] // groups
    return [
        (
            quant[:, b * width : (b + 1) * width].astype(F32)
            * jnp.broadcast_to(scales[b : b + 1], (width, rows)).T
        ).astype(BF16)
        for b in range(groups)
    ]


def reduced_rows(prior, tokens):
    wide = lax.dot_general(tokens, prior, NN, preferred_element_type=F32)
    half = (wide[:, :128] + wide[:, 128:]).T
    return half[:64] + half[64:]


def begin(count, *makers):
    def one(i, carry):
        for make in makers:
            make(i).start()
        return carry

    lax.fori_loop(0, count, one, 0)


def widths(width_ref, n_tile):
    tile = lax.axis_index("tile")
    number = lax.axis_index("region") * n_tile + tile
    left = jnp.where(tile > 0, width_ref[number], 0)
    last = width_ref.shape[0] - 1
    right = jnp.where(tile < n_tile - 1, width_ref[jnp.minimum(number + 1, last)], 0)
    return left, right


def band_kernel(valid_ref, head_ref, tail_ref, head_s_ref, tail_s_ref, prior_ref,
                forward_ref, backward_ref, prior3_ref, head_out_ref, tail_out_ref, *, tok_rows):
    high, mid, low = split3(prior_ref[...])
    prior = jnp.concatenate([high, mid, low, jnp.zeros_like(low)], 0).T
    prior3_ref[...] = prior
    head = jnp.concatenate(dequantize(head_ref[...], head_s_ref[...]), 1)
    head_out_ref[...] = head
    backward_ref[: high.shape[0], :] = reduced_rows(prior, head)
    backward_ref[high.shape[0] :, :] = jnp.zeros((ROWS - high.shape[0], BAND), F32)
    tail = jnp.concatenate(dequantize(tail_ref[...], tail_s_ref[...]), 1)
    tail_out_ref[...] = tail
    keep = high.shape[0]
    forward_ref[:keep, :] = reduced_rows(prior, tail)
    place = tok_rows - BAND + lax.broadcasted_iota(jnp.int32, (ROWS - keep, BAND), 1)
    forward_ref[keep:, :] = jnp.where(place < valid_ref[0], 2.0, 1.0)


def bulk_kernel(width_ref, valid_ref, quant_ref, scale_ref, prior3_ref,
                token_ref, sum_ref, raw_ref, held_ref, in_sem, out_sem, *, tok_rows, n_tile):
    steps = tok_rows // STEP
    chunks = [pl.ds(step * STEP, STEP) for step in range(steps)]
    part = STEP // 2

    def mover(source, target, sems, step):
        def make(i):
            rows = pl.ds(pl.multiple_of(step * STEP + i * part, part), part)
            return pltpu.make_async_copy(source.at[rows], target.at[rows], sems.at[2 * step + i])

        return make

    arrive = [mover(quant_ref, raw_ref, in_sem, step) for step in range(steps)]
    leave = [mover(held_ref, token_ref, out_sem, step) for step in range(steps)]
    begin(2, arrive[0])
    begin(2, arrive[1])
    left, right = widths(width_ref, n_tile)
    for step in range(steps + 1):
        if step < steps:
            for i in range(2):
                arrive[step](i).wait()
        makers = [leave[step - 1]] if step > 0 else []
        if step + 2 < steps:
            makers.append(arrive[step + 2])
        if makers:
            begin(2, *makers)
        if step < steps:
            blocks = dequantize(raw_ref[chunks[step], :], scale_ref[:, chunks[step]])
            for b, block in enumerate(blocks):
                held_ref[chunks[step], b * block.shape[1] : (b + 1) * block.shape[1]] = block
        if step > 0:
            tokens = held_ref[chunks[step - 1], :]
            reduced = reduced_rows(prior3_ref[...], tokens)
            place = (step - 1) * STEP + lax.broadcasted_iota(jnp.int32, (1, STEP), 1)
            inner = (place >= left) & (place < tok_rows - right) & (place < valid_ref[0])
            weight = jnp.where(inner, 1.0, 0.0)
            reduced = reduced * weight
            high = reduced.astype(BF16)
            low = (reduced - high.astype(F32)).astype(BF16)
            extra = jnp.broadcast_to(weight, (16, STEP)).astype(BF16)
            total = lax.dot_general(
                jnp.concatenate([high, low, extra], 0), tokens, NN, preferred_element_type=F32
            )
            sum_ref[...] = total if step == 1 else sum_ref[...] + total
    for copies in leave:
        for i in range(2):
            copies(i).wait()


def join_kernel(width_ref, valid_ref, head_ref, tail_ref, sum_ref, forward_ref, backward_ref,
                before_ref, after_ref, out_ref, *, tok_rows, n_tile):
    left, right = widths(width_ref, n_tile)
    keep = sum_ref.shape[0] // 2 - 8
    place = lax.broadcasted_iota(jnp.int32, (1, BAND), 1)
    before = pltpu.roll(before_ref[...], lax.rem(left, BAND), 1)
    after = pltpu.roll(after_ref[...], lax.rem(BAND - right, BAND), 1)
    count = jnp.where(place < left, before[keep : keep + 1], 0.0)
    head = (backward_ref[:keep, :] + before[:keep]) * (count * 0.25)
    both = jnp.where(place >= BAND - right, forward_ref[keep : keep + 1, :], 0.0)
    tail = (forward_ref[:keep, :] + after[:keep]) * (both * 0.25)
    total = sum_ref[...]
    for reduced, weight, rows in ((head, count, head_ref), (tail, both, tail_ref)):
        reduced = jnp.where(weight > 0.0, reduced, 0.0)
        high = reduced.astype(BF16)
        low = (reduced - high.astype(F32)).astype(BF16)
        extra = jnp.broadcast_to(weight * 0.5, (16, BAND)).astype(BF16)
        total = total + lax.dot_general(
            jnp.concatenate([high, low, extra], 0), rows[...], NN, preferred_element_type=F32
        )
    update = total[:keep] + total[keep : 2 * keep]
    row = lax.broadcasted_iota(jnp.int32, (8, 128), 0)
    parts = out_ref.shape[0]
    share = total.shape[1] // 128 // parts
    for part in range(parts):
        extra = jnp.where(row == share, valid_ref[0].astype(F32), 0.0)
        for c in range(share):
            lanes = slice((part * share + c) * 128, (part * share + c + 1) * 128)
            out_ref[part, c * keep : (c + 1) * keep, :] = update[:, lanes]
            extra = jnp.where(row == c, total[2 * keep : 2 * keep + 1, lanes], extra)
        out_ref[part, share * keep :, :] = extra


def inverse_factor(square):
    size = square.shape[0]
    eye = (
        lax.broadcasted_iota(jnp.int32, (size, size), 0)
        == lax.broadcasted_iota(jnp.int32, (size, size), 1)
    ).astype(F32)
    both = jnp.concatenate([square, eye], 1)
    wide = (8, 2 * size)
    groups = size // 8
    rows = [both[8 * i : 8 * i + 8] for i in range(groups)]
    sublane = lax.broadcasted_iota(jnp.int32, wide, 0)
    done = []
    for j in range(groups):
        columns = [
            [jnp.broadcast_to(rows[i][:, 8 * j + k : 8 * j + k + 1], wide) for i in range(j, groups)]
            for k in range(8)
        ]
        scale = jnp.zeros(wide, F32)
        for k in range(8):
            pivot = jnp.broadcast_to(columns[k][0][k : k + 1], wide)
            scale = jnp.where(sublane == k, lax.rsqrt(pivot), scale)
            line = jnp.broadcast_to(rows[j][k : k + 1], wide) / pivot
            ratio = [
                jnp.broadcast_to(columns[k][0][m : m + 1], wide) / pivot for m in range(k + 1, 8)
            ]
            for i in range(j, groups):
                factor = columns[k][i - j]
                if i == j:
                    factor = jnp.where(sublane > k, factor, 0.0)
                rows[i] = rows[i] - factor * line
                for m in range(k + 1, 8):
                    columns[m][i - j] = columns[m][i - j] - factor * ratio[m - k - 1]
        done.append(rows[j] * scale)
    return jnp.concatenate(done, 0)[:, size:]


def basis_kernel(own_ref, other_ref, prior_ref, head_ref, tail_ref, far_ref,
                 basis_ref, pair_ref, shift_ref, head_out_ref, tail_out_ref, token_ref, sem):
    size = token_ref.shape[0] // sem.shape[0]

    def fetch(i):
        rows = pl.ds(pl.multiple_of(i * size, size), size)
        return pltpu.make_async_copy(far_ref.at[rows], token_ref.at[rows], sem.at[i])

    begin(sem.shape[0], fetch)
    core = lax.rem(lax.axis_index("region"), 2)
    keep = prior_ref.shape[0]
    share = prior_ref.shape[1] // 256
    own, other = own_ref[...], other_ref[...]
    halves = [jnp.where(core == part, own, other) for part in range(2)]
    update = jnp.concatenate([half[c * keep : (c + 1) * keep] for half in halves for c in range(share)], 1)
    base = share * keep
    sums = jnp.concatenate([half[base + c : base + c + 1] for half in halves for c in range(share)], 1)
    count = own[base + share : base + share + 1, :1]
    average = sums / count
    image = jnp.sum(prior_ref[...] * average, axis=1, keepdims=True)
    update = update - image * sums
    square = lax.dot_general(update, update, NT, precision=lax.Precision.HIGHEST, preferred_element_type=F32)
    inverse = inverse_factor(square)
    basis = lax.dot_general(inverse, update, NN, precision=lax.Precision.HIGHEST, preferred_element_type=F32)
    basis_ref[...] = basis
    high = basis.astype(BF16)
    low = (basis - high.astype(F32)).astype(BF16)
    pair = jnp.concatenate([high, low], 0).T
    pair_ref[...] = pair
    shift_ref[...] = jnp.broadcast_to(jnp.sum(basis * average, axis=1, keepdims=True), shift_ref.shape)
    for rows, out in ((head_ref, head_out_ref), (tail_ref, tail_out_ref)):
        wide = lax.dot_general(rows[...], pair, NN, preferred_element_type=F32).T
        out[...] = wide[:keep] + wide[keep:]
    for i in range(sem.shape[0]):
        fetch(i).wait()


def project_kernel(valid_ref, token_ref, pair_ref, shift_ref, basis_ref,
                   out_ref, basis_out_ref, value_ref, out_sem, *, tok_rows):
    keep = shift_ref.shape[0]
    steps = tok_rows // STEP
    leave = [pltpu.make_async_copy(basis_ref, basis_out_ref, out_sem.at[steps])]
    leave[0].start()
    for step in range(steps):
        lanes = pl.ds(step * STEP, STEP)
        wide = lax.dot_general(token_ref[lanes, :], pair_ref[...], NN, preferred_element_type=F32).T
        place = step * STEP + lax.broadcasted_iota(jnp.int32, (1, STEP), 1)
        value = wide[:keep] + wide[keep:] - shift_ref[:, :1]
        value_ref[:, lanes] = jnp.where(place < valid_ref[0], value, 0.0)
        leave.append(pltpu.make_async_copy(value_ref.at[:, lanes], out_ref.at[:, lanes], out_sem.at[step]))
        if step > 0:
            leave[step].start()
    leave[steps].start()
    for copy in leave:
        copy.wait()


def blend_kernel(width_ref, valid_ref, head_ref, tail_ref, before_ref, after_ref, shift_ref,
                 whole_ref, out_ref, buffer_ref, sem_ref, *, tok_rows, n_tile):
    left, right = widths(width_ref, n_tile)
    place = lax.broadcasted_iota(jnp.int32, (1, BAND), 1)
    shift = shift_ref[:, :1]
    before = pltpu.roll(before_ref[...], lax.rem(left, BAND), 1)
    after = pltpu.roll(after_ref[...], lax.rem(BAND - right, BAND), 1)
    head = jnp.where(place < left, (head_ref[...] + before) * 0.5, head_ref[...]) - shift
    tail = jnp.where(place >= BAND - right, (tail_ref[...] + after) * 0.5, tail_ref[...]) - shift
    start = tok_rows - BAND
    buffer_ref[0] = jnp.where(place < valid_ref[0], head, 0.0)
    buffer_ref[1] = jnp.where(start + place < valid_ref[0], tail, 0.0)
    first = pltpu.make_async_copy(buffer_ref.at[0], out_ref.at[:, pl.ds(0, BAND)], sem_ref.at[0])
    second = pltpu.make_async_copy(buffer_ref.at[1], out_ref.at[:, pl.ds(start, BAND)], sem_ref.at[1])
    first.start()
    second.start()
    first.wait()
    second.wait()


def smem():
    return pl.BlockSpec(memory_space=pltpu.SMEM)


def near():
    return pl.BlockSpec(memory_space=pltpu.VMEM)


def far():
    return pl.BlockSpec(memory_space=pltpu.HBM)


def params(mib):
    return pltpu.CompilerParams(vmem_limit_bytes=mib << 20)


def flip(value, masks):
    pairs = [(g, g ^ masks[(g >> 5) & 1]) for g in range(128)]
    return lax.ppermute(value, AXES, pairs)


def exchange(tail, head):
    count = lax.axis_size("tile")
    even = lax.axis_index("tile") % 2 == 0
    far_pairs = [(i, i + 1) for i in range(1, count - 1, 2)]
    far_pairs += [(j, i) for i, j in far_pairs]
    inner = lax.ppermute(jnp.where(even, tail, head), "tile", [(i, i ^ 1) for i in range(count)])
    outer = lax.ppermute(jnp.where(even, head, tail), "tile", far_pairs)
    return jnp.where(even, outer, inner), jnp.where(even, inner, outer)


def pick(stack, index):
    return lax.dynamic_index_in_dim(stack, index, 0, keepdims=False)


def reduce_all(halves):
    core = lax.axis_index("region") % 2
    both = (32, 32)
    mine = pick(halves, core) + flip(pick(halves, 1 - core), both)
    along_y, along_x, along_z = (2, 4, 6), (8, 16, 24), (1, 64, 65)
    for stage in ((along_y, along_x), (along_x, along_z), (along_z, along_y)):
        near_one, far_one, across = [flip(mine, masks) for masks in zip(*stage)]
        mine = (mine + near_one) + (far_one + across)
    return mine, flip(mine, both)


def per_device(quantized, block_scales, band_width, valid_count, prior_basis):
    tok_rows, feat_dim = quantized.shape
    keep = prior_basis.shape[1]
    groups = block_scales.shape[0]
    n_tile = lax.axis_size("tile")
    steps = tok_rows // STEP
    last = tok_rows // BAND - 1
    head_rows = pl.BlockSpec((BAND, feat_dim), lambda i: (0, 0))
    tail_rows = pl.BlockSpec((BAND, feat_dim), lambda i: (last, 0))

    def whole(*shape):
        return pl.BlockSpec(shape, lambda i: (0,) * len(shape))

    quant_far = pltpu.with_memory_space_constraint(quantized, pltpu.HBM)
    prior = prior_basis.T
    prior_far = pltpu.with_memory_space_constraint(prior, pltpu.HBM)
    scales_far = pltpu.with_memory_space_constraint(block_scales, pltpu.HBM)
    forward, backward, prior3, head_tokens, tail_tokens = pl.pallas_call(
        functools.partial(band_kernel, tok_rows=tok_rows),
        grid=(1,),
        in_specs=[
            smem(),
            head_rows,
            tail_rows,
            pl.BlockSpec((groups, BAND), lambda i: (0, 0)),
            pl.BlockSpec((groups, BAND), lambda i: (0, last)),
            whole(keep, feat_dim),
        ],
        out_specs=[
            whole(ROWS, BAND),
            whole(ROWS, BAND),
            whole(feat_dim, 4 * keep),
            whole(BAND, feat_dim),
            whole(BAND, feat_dim),
        ],
        out_shape=[
            jax.ShapeDtypeStruct((ROWS, BAND), F32),
            jax.ShapeDtypeStruct((ROWS, BAND), F32),
            jax.ShapeDtypeStruct((feat_dim, 4 * keep), BF16),
            jax.ShapeDtypeStruct((BAND, feat_dim), BF16),
            jax.ShapeDtypeStruct((BAND, feat_dim), BF16),
        ],
        compiler_params=params(24),
        name="band",
    )(valid_count, quant_far, quant_far, scales_far, scales_far, prior_far)
    before, after = exchange(forward, backward)
    bulk = pl.pallas_call(
        functools.partial(bulk_kernel, tok_rows=tok_rows, n_tile=n_tile),
        in_specs=[smem(), smem(), far(), near(), near()],
        out_specs=[far(), near()],
        out_shape=[
            pltpu.HBM((tok_rows, feat_dim), BF16),
            jax.ShapeDtypeStruct((2 * keep + 16, feat_dim), F32),
        ],
        scratch_shapes=[
            pltpu.VMEM((tok_rows, feat_dim), BF16),
            pltpu.VMEM((tok_rows, feat_dim), BF16),
            pltpu.SemaphoreType.DMA((2 * steps,)),
            pltpu.SemaphoreType.DMA((2 * steps,)),
        ],
        compiler_params=params(32),
        name="bulk",
    )
    tokens, sums = bulk(band_width, valid_count, quant_far, block_scales, prior3)
    pieces = pl.pallas_call(
        functools.partial(join_kernel, tok_rows=tok_rows, n_tile=n_tile),
        grid=(1,),
        in_specs=[
            smem(),
            smem(),
            whole(BAND, feat_dim),
            whole(BAND, feat_dim),
            whole(2 * keep + 16, feat_dim),
            whole(ROWS, BAND),
            whole(ROWS, BAND),
            whole(ROWS, BAND),
            whole(ROWS, BAND),
        ],
        out_specs=whole(2, feat_dim // 256 * keep + 8, 128),
        out_shape=jax.ShapeDtypeStruct((2, feat_dim // 256 * keep + 8, 128), F32),
        compiler_params=params(24),
        name="join",
    )(band_width, valid_count, head_tokens, tail_tokens, sums, forward, backward, before, after)
    own, other = reduce_all(pieces)
    tokens = pltpu.with_memory_space_constraint(tokens, pltpu.HBM)
    basis, pair, shift, head, tail, early = pl.pallas_call(
        basis_kernel,
        in_specs=[near()] * 5 + [far()],
        out_specs=[near()] * 6,
        out_shape=[
            jax.ShapeDtypeStruct((keep, feat_dim), F32),
            jax.ShapeDtypeStruct((feat_dim, 2 * keep), BF16),
            jax.ShapeDtypeStruct((keep, 128), F32),
            jax.ShapeDtypeStruct((keep, BAND), F32),
            jax.ShapeDtypeStruct((keep, BAND), F32),
            jax.ShapeDtypeStruct((tok_rows, feat_dim), BF16),
        ],
        scratch_shapes=[pltpu.SemaphoreType.DMA((8,))],
        compiler_params=params(24),
        name="basis",
    )(own, other, prior, head_tokens, tail_tokens, tokens)
    before, after = exchange(tail, head)
    raw, basis = pl.pallas_call(
        functools.partial(project_kernel, tok_rows=tok_rows),
        in_specs=[smem(), near(), near(), near(), near()],
        out_specs=[far(), far()],
        out_shape=[pltpu.HBM((keep, tok_rows), F32), pltpu.HBM((keep, feat_dim), F32)],
        scratch_shapes=[
            pltpu.VMEM((keep, tok_rows), F32),
            pltpu.SemaphoreType.DMA((steps + 1,)),
        ],
        compiler_params=params(24),
        name="project",
    )(valid_count, early, pair, shift, basis)
    projected = pl.pallas_call(
        functools.partial(blend_kernel, tok_rows=tok_rows, n_tile=n_tile),
        in_specs=[smem(), smem()]
        + [pl.BlockSpec(memory_space=pltpu.VMEM)] * 5
        + [pl.BlockSpec(memory_space=pl.ANY)],
        out_specs=pl.BlockSpec(memory_space=pl.ANY),
        out_shape=jax.ShapeDtypeStruct((keep, tok_rows), F32),
        scratch_shapes=[pltpu.VMEM((2, keep, BAND), F32), pltpu.SemaphoreType.DMA((2,))],
        input_output_aliases={7: 0},
        compiler_params=params(8),
        name="blend",
    )(band_width, valid_count, head, tail, before, after, shift, raw)
    return projected, basis.T


def solution(mesh):
    return jax.shard_map(
        per_device,
        mesh=mesh,
        in_specs=(
            P(("region", "tile"), None),
            P(None, ("region", "tile")),
            P(),
            P(("region", "tile")),
            P(),
        ),
        out_specs=(P(None, ("region", "tile")), P()),
        check_vma=False,
    )
```
